32 devices in a mesh: seq: 8 (over z, x), head: 4 (over y, core).
Axes of the slice: x: 2, y: 2, z: 4, core: 2. Of those that a mesh axis runs over, the one named last changes fastest.
Arguments:
- queries: bfloat16 [2048, 2048], P('seq', 'head'), may hold values from -8 to 8
- keys: bfloat16 [2048, 512], P('seq', 'head'), may hold values from -4 to 4
- values: bfloat16 [2048, 512], P('seq', 'head'), may hold values from -6 to 6
- doc_ids: int32 [2048], replicated, may hold values from 0 to 15, never falling along the last dimension, each value on 1 to 1024 neighbouring positions
- span_order: int32 [16], replicated, may hold values from 0 to 15, each once
- out_weight: bfloat16 [2048, 4096], P('head', 'seq'), may hold values from -0.1875 to 0.1875
Outputs:
- layer_out: bfloat16 [2048, 4096], P('seq', 'head')
The draws below stay inside these ranges and needn't reach their ends.
All inputs are finite; a program needn't handle non-finite values.
Results may differ from the reference program's by a relative error of at most 0.012.
Values may be sent and summed in bfloat16 or wider, within the bound.
No kernel may reach another device: no remote copies, remote signals or barrier semaphores. Data moves between devices by JAX's collectives and lax.ppermute only.
A program may use at most 64 MiB of HBM per device.

```python
import math
import jax
import jax.numpy as jnp
import numpy as np
from jax import lax

D = 4096
HEADS = 16
KV_HEADS = 4
DH = 128
GROUP = 4
TOK_DEV = 256
SEQ = 2048
DOCS = 16
MAX_DOC = 1024
N_SEQ = 8


def draw_queries(key, part):
    base = jnp.clip(jax.random.normal(jax.random.fold_in(key, 11), (SEQ, HEADS * DH), jnp.float32), -4.0, 4.0)
    return base.astype(jnp.bfloat16)


def draw_keys(key, part):
    base = jnp.clip(jax.random.normal(jax.random.fold_in(key, 21), (SEQ, KV_HEADS * DH), jnp.float32), -4.0, 4.0)
    return base.astype(jnp.bfloat16)


def spiked(result, key, source, target, parts, factor):
    owner, partner = [(jnp.arange(result.shape[dim]) // (result.shape[dim] // parts)).reshape([-1 if axis == dim else 1 for axis in range(result.ndim)]) for dim in (source, target)]
    chosen = jax.random.permutation(key, parts)[partner]
    strong = (owner == chosen) | (owner == (partner + parts // 2) % parts)
    return jnp.where(strong, factor * result, result)


def block_scale(own_key, shape, pieces, least, high):
    def one(axis_at, shards_of):
        steps = jax.random.uniform(jax.random.fold_in(jax.random.fold_in(own_key, 6), axis_at), (shards_of,), jnp.float32, least / len(pieces), high / len(pieces))
        return jnp.repeat(jnp.exp(steps), shape[axis_at] // shards_of).reshape((-1,) + (1,) * (len(shape) - axis_at - 1))

    level = one(*pieces[0])
    for cut in pieces[1:]:
        level = level * one(*cut)
    return level


def length_profile(amount, total, limit, lean):
    loads = [(1 << 20) // math.isqrt(grade ** lean) + 1 for grade in range(2, amount + 1)]
    surplus, given = total - limit - (amount - 1), [1] * (amount - 1)
    while surplus > 0:
        candidates = [i for i in range(amount - 1) if given[i] < limit]
        whole, remaining = sum([loads[i] for i in candidates]), surplus
        for i in candidates:
            more = min(limit - given[i], max(1, remaining * loads[i] // whole), surplus)
            given[i] = given[i] + more
            surplus = surplus - more
    return np.array([limit] + given)


def ragged_sizes(stream_key, amount, total, most, lean):
    if amount == 2:
        one = jax.random.randint(stream_key, (), max(1, total - most), min(most, total - 1) + 1)
        return jnp.stack([one, total - one])
    tallies = jnp.asarray(length_profile(amount, total, most, lean), jnp.int32)
    pairs = (amount - 1) // 2
    donor, taker = tallies[1:1 + 2 * pairs:2], tallies[2:2 + 2 * pairs:2]
    slack = jnp.minimum(donor - 1, most - taker)
    shifted = jax.random.randint(jax.random.fold_in(stream_key, 1), (pairs,), 0, 1 << 20) % (slack + 1)
    tallies = tallies.at[1:1 + 2 * pairs:2].set(donor - shifted).at[2:2 + 2 * pairs:2].set(taker + shifted)
    return tallies[jax.random.permutation(jax.random.fold_in(stream_key, 2), amount)]


def centred(rng, dims, width, bound, cuts=(), kind=jnp.bfloat16):
    entries = jax.random.normal(rng, dims, jnp.float32) * width
    if len(cuts) > 0:
        entries = block_scale(rng, dims, cuts, -0.22, 0.18) * entries
    return jnp.clip(entries, min=-bound, max=bound).astype(kind)


def noise_with(own_key, shape, spread, reach, split, heavy, kind=jnp.bfloat16):
    values = spread * jax.random.normal(own_key, shape, jnp.float32)
    if split:
        values = values * block_scale(own_key, shape, split, -0.22, 0.18)
    return jnp.clip(spiked(values, jax.random.fold_in(own_key, 3), *heavy), -reach, reach).astype(kind)


def setup_inputs(seed: int = 0) -> dict:
    arg_keys = jax.random.split(jax.random.key(seed), 7)
    return {
        "queries": draw_queries(jax.random.fold_in(arg_keys[6], 71), 0),
        "keys": draw_keys(jax.random.fold_in(arg_keys[6], 71), 0),
        "values": centred(arg_keys[2], (SEQ, KV_HEADS * DH), 1.0, 6.0, ((0, 8), (1, 4))),
        "doc_ids": jnp.searchsorted(jnp.cumsum(ragged_sizes(arg_keys[3], DOCS, SEQ, MAX_DOC, 2)), jnp.arange(SEQ), side="right").astype(jnp.int32),
        "span_order": jax.random.permutation(arg_keys[4], 2 * N_SEQ).astype(jnp.int32),
        "out_weight": noise_with(arg_keys[5], (HEADS * DH, D), (HEADS * DH) ** -0.5, 0.1875, ((0, 4), (1, 8)), (0, 1, 8, 2.0)),
    }


def reference(queries, keys, values, doc_ids, span_order, out_weight):
    span = TOK_DEV // 2
    rows = jnp.arange(SEQ, dtype=jnp.int32)
    pos = (span_order[rows // span] * span + rows % span).astype(jnp.int32)
    doc = doc_ids[pos]
    scale = 1.0 / math.sqrt(DH)
    key_all = keys.reshape(SEQ, KV_HEADS, DH).astype(jnp.float32)
    val_all = values.reshape(SEQ, KV_HEADS, DH).astype(jnp.float32)
    block = math.gcd(SEQ, 128)

    def one_block(index):
        start = (index * block).astype(jnp.int32)
        qblk = lax.dynamic_slice_in_dim(queries, start, block, 0)
        qblk = qblk.reshape(block, KV_HEADS, GROUP, DH).astype(jnp.float32)
        qpos = lax.dynamic_slice_in_dim(pos, start, block, 0)
        qdoc = lax.dynamic_slice_in_dim(doc, start, block, 0)
        scores = jnp.einsum('qhgd,khd->hgqk', qblk, key_all) * scale
        visible = (qdoc[:, None] == doc[None, :]) & (pos[None, :] <= qpos[:, None])
        masked = jnp.where(visible, scores, jnp.float32(-1e+30))
        largest = lax.optimization_barrier(jnp.max(masked, axis=-1, keepdims=True))
        weights = jnp.where(visible, jnp.exp(masked - largest), jnp.float32(0.0))
        total = lax.optimization_barrier(jnp.sum(weights, axis=-1))
        weights_b = weights.astype(jnp.bfloat16).astype(jnp.float32)
        summed = jnp.einsum('hgqk,khd->qhgd', weights_b, val_all)
        attended = summed / jnp.transpose(total, (2, 0, 1))[..., None]
        return attended.astype(jnp.bfloat16).reshape(block, HEADS * DH)
    attended = lax.map(one_block, jnp.arange(SEQ // block, dtype=jnp.int32))
    attended = attended.reshape(SEQ, HEADS * DH)
    return jnp.dot(attended, out_weight, preferred_element_type=jnp.float32).astype(jnp.bfloat16)
```

```python
import functools
import math

import jax
import jax.numpy as jnp
from jax import lax
from jax.experimental import pallas as pl
from jax.experimental.pallas import tpu as pltpu
from jax.sharding import PartitionSpec as P

DH = 128
LANES = 128
VMEM = pl.BlockSpec(memory_space=pltpu.VMEM)
SMEM = pl.BlockSpec(memory_space=pltpu.SMEM)


def ring_order(n):
    return list(range(0, n, 2)) + list(range(n - 1, 0, -2))


def ring_tables(n):
    ring = ring_order(n)
    place = {s: i for i, s in enumerate(ring)}
    forward = [(ring[i], ring[(i + 1) % n]) for i in range(n)]
    backward = [(b, a) for a, b in forward]
    sources = []
    for s in range(n):
        row = [s]
        for hop in range(1, n // 2):
            row.append(ring[(place[s] - hop) % n])
            row.append(ring[(place[s] + hop) % n])
        row.append(ring[(place[s] + n // 2) % n])
        sources.append(row)
    return forward, backward, sources


def attention_kernel(
    n, span, group, src_ref, order_ref, first_ref, docs_ref, q_ref, *rest
):
    kv_refs, (out_ref, s_ref, m_ref, l_ref, acc_ref) = rest[:n], rest[n:]
    base2 = math.log2(math.e) / math.sqrt(DH)
    mine = src_ref[0]
    dims = (((1,), (1,)), ((), ()))

    for part in range(2):
        rows = pl.ds(part * span, span)
        qpos = order_ref[2 * mine + part]
        q = jnp.concatenate(
            [q_ref[rows, h * DH : (h + 1) * DH] for h in range(group)], axis=0
        )
        qdoc = jnp.transpose(
            jnp.broadcast_to(docs_ref[pl.ds(qpos, 1), :], (span, span)).astype(jnp.float32)
        )
        qfirst = first_ref[qpos * span]
        ahead = lax.broadcasted_iota(jnp.int32, (span, span), 1) - lax.broadcasted_iota(
            jnp.int32, (span, span), 0
        )
        m_ref[...] = jnp.full_like(m_ref, -1e30)
        l_ref[...] = jnp.zeros_like(l_ref)
        acc_ref[...] = jnp.zeros_like(acc_ref)

        def seen(j):
            kpos = order_ref[2 * src_ref[j // 2] + j % 2]
            return kpos, (kpos <= qpos) & (first_ref[kpos * span + span - 1] >= qfirst)

        for j in range(2 * n):
            kpos, live = seen(j)

            @pl.when(live)
            def _():
                k = kv_refs[j // 2][(j % 2) * span : (j % 2 + 1) * span, :DH]
                s = lax.dot_general(q, k, dims, preferred_element_type=jnp.float32)
                kdoc = docs_ref[pl.ds(kpos, 1), :].astype(jnp.float32)
                visible = (qdoc == kdoc) & (ahead <= (qpos - kpos) * span)
                s = jnp.where(visible[None], s.reshape(group, span, span), -1e30)
                s = s.reshape(group * span, span)
                s_ref[:, j * span : (j + 1) * span] = s
                m_ref[...] = jnp.maximum(m_ref[...], s)

        largest = jnp.max(m_ref[...], axis=1, keepdims=True) * base2

        for j in range(2 * n):
            kpos, live = seen(j)

            @pl.when(live)
            def _():
                p = jnp.exp2(s_ref[:, j * span : (j + 1) * span] * base2 - largest)
                l_ref[...] += p
                v = kv_refs[j // 2][(j % 2) * span : (j % 2 + 1) * span, DH:]
                acc_ref[...] += jnp.dot(
                    p.astype(jnp.bfloat16), v, preferred_element_type=jnp.float32
                )

        total = jnp.sum(l_ref[...], axis=1, keepdims=True)
        attended = (acc_ref[...] / total).astype(jnp.bfloat16)
        for h in range(group):
            out_ref[rows, h * DH : (h + 1) * DH] = attended[h * span : (h + 1) * span]


def project_kernel(pieces, slot_ref, half_ref, a_ref, *rest):
    w_refs, out_ref = rest[:-1], rest[-1]
    a = a_ref[...]
    for i, w_ref in enumerate(w_refs):
        block, piece = pieces[i]
        width = w_ref.shape[1]
        start = pl.multiple_of(half_ref[block] + piece * width, LANES)
        c = jnp.dot(a, w_ref[...], preferred_element_type=jnp.float32)
        out_ref[slot_ref[block], :, pl.ds(start, width)] = c.astype(jnp.bfloat16)


def ring_device(n, heads, queries, keys, values, doc_ids, span_order, out_weight):
    tok_rows = queries.shape[0]
    span = tok_rows // 2
    group = queries.shape[1] // DH
    width = out_weight.shape[1]
    forward, backward, sources = ring_tables(n)
    mine = lax.axis_index("seq")
    head = lax.axis_index("head")
    src = lax.dynamic_index_in_dim(jnp.asarray(sources, jnp.int32), mine, 0, False)

    def gather(pieces):
        ups, downs = list(pieces), list(pieces)
        late = (len(pieces) + 1) // 2
        got = [list(pieces)]
        for hop in range(1, n // 2 + 1):
            last = hop == n // 2
            for i in range(len(pieces)):
                if not last or i < late:
                    ups[i] = lax.ppermute(ups[i], "seq", forward)
                if not last or i >= late:
                    downs[i] = lax.ppermute(downs[i], "seq", backward)
            if last:
                got.append(ups[:late] + downs[late:])
            else:
                got.append(list(ups))
                got.append(list(downs))
        return got

    kv = [g[0] for g in gather([jnp.concatenate([keys, values], axis=1)])]
    split = 2
    w = gather([out_weight[:, i * width // split : (i + 1) * width // split] for i in range(split)])

    attended = pl.pallas_call(
        functools.partial(attention_kernel, n, span, group),
        out_shape=jax.ShapeDtypeStruct((tok_rows, group * DH), jnp.bfloat16),
        in_specs=[SMEM, SMEM, SMEM] + [VMEM] * (2 + n),
        out_specs=VMEM,
        scratch_shapes=[
            pltpu.VMEM((group * span, 2 * n * span), jnp.float32),
            pltpu.VMEM((group * span, span), jnp.float32),
            pltpu.VMEM((group * span, span), jnp.float32),
            pltpu.VMEM((group * span, DH), jnp.float32),
        ],
        cost_estimate=pl.CostEstimate(
            flops=4 * group * tok_rows * n * tok_rows * DH,
            bytes_accessed=n * tok_rows * 4 * DH,
            transcendentals=group * tok_rows * n * tok_rows,
        ),
        name="attention",
    )(src, span_order, doc_ids, doc_ids.reshape(-1, span), queries, *kv)

    per = n // heads
    slot = head ^ (src // per)
    half = (src % per) * width
    pieces = [(b, i) for b in range(n) for i in range(split)]
    partial = pl.pallas_call(
        functools.partial(project_kernel, pieces),
        out_shape=jax.ShapeDtypeStruct((heads, tok_rows, per * width), jnp.bfloat16),
        in_specs=[SMEM, SMEM] + [VMEM] * (1 + len(pieces)),
        out_specs=VMEM,
        cost_estimate=pl.CostEstimate(
            flops=2 * tok_rows * group * DH * n * width,
            bytes_accessed=group * DH * n * width * 2,
            transcendentals=0,
        ),
        name="project",
    )(slot, half, attended, *[w[b][i] for b, i in pieces])

    sums = [partial[k].astype(jnp.float32) for k in range(heads)]
    step = 1
    while step < heads:
        pairs = [(h, h ^ step) for h in range(heads)]
        keep = list(range(0, heads, 2 * step))
        got = [lax.ppermute(sums[k | step].astype(jnp.bfloat16), "head", pairs) for k in keep]
        for k, other in zip(keep, got):
            sums[k] = sums[k] + other.astype(jnp.float32)
        step *= 2
    return sums[0].astype(jnp.bfloat16)


def on_device(queries, keys, values, doc_ids, span_order, out_weight):
    tok_rows = queries.shape[0]
    span = tok_rows // 2
    local_heads = queries.shape[1] // DH
    local_kv = keys.shape[1] // DH
    group_size = local_heads // local_kv
    n_blocks = span_order.shape[0]
    scale = 1.0 / math.sqrt(DH)
    mine = lax.axis_index("seq")
    own_blocks = lax.dynamic_slice_in_dim(span_order, 2 * mine, 2, 0)
    local_rows = jnp.arange(tok_rows, dtype=jnp.int32)
    qpos = jnp.where(local_rows < span, own_blocks[0], own_blocks[1]) * span + local_rows % span
    qdoc = jnp.take(doc_ids, qpos)
    q_heads = queries.reshape(tok_rows, local_kv, group_size, DH)

    def update(state, kblk, vblk, kpos, kdoc):
        largest, total, summed = state
        count = kblk.shape[0]
        k_heads = kblk.reshape(count, local_kv, DH)
        v_heads = vblk.reshape(count, local_kv, DH)
        scores = (
            jnp.einsum("qhgd,khd->hgqk", q_heads, k_heads, preferred_element_type=jnp.float32)
            * scale
        )
        visible = (qdoc[:, None] == kdoc[None, :]) & (kpos[None, :] <= qpos[:, None])
        masked = jnp.where(visible, scores, jnp.float32(-1e30))
        new_largest = jnp.maximum(largest, jnp.max(masked, axis=-1))
        factor = jnp.exp(largest - new_largest)
        weights = jnp.where(visible, jnp.exp(masked - new_largest[..., None]), jnp.float32(0.0))
        total = total * factor + jnp.sum(weights, axis=-1)
        weights_b = weights.astype(jnp.bfloat16)
        added = jnp.einsum("hgqk,khd->qhgd", weights_b, v_heads, preferred_element_type=jnp.float32)
        summed = summed * jnp.transpose(factor, (2, 0, 1))[..., None] + added
        return (new_largest, total, summed)

    initial = (
        jnp.full((local_kv, group_size, tok_rows), -1e30, jnp.float32),
        jnp.zeros((local_kv, group_size, tok_rows), jnp.float32),
        jnp.zeros((tok_rows, local_kv, group_size, DH), jnp.float32),
    )
    state = initial
    kpiece = lax.all_gather(keys, "seq", axis=0, tiled=True)
    vpiece = lax.all_gather(values, "seq", axis=0, tiled=True)
    count = kpiece.shape[0]
    width = math.gcd(count, 1024)
    steps = count // width
    rows = jnp.arange(count, dtype=jnp.int32)
    match = (rows // span)[:, None] == jnp.arange(n_blocks, dtype=jnp.int32)[None, :]
    owner = jnp.sum(jnp.where(match, span_order[None, :], 0), axis=1)
    kpos = owner * span + rows % span
    kdoc = jnp.take(doc_ids, kpos)
    kparts = kpiece.reshape(steps, width, kpiece.shape[1])
    vparts = vpiece.reshape(steps, width, vpiece.shape[1])

    def one_step(carry, items):
        kblk, vblk, pblk, dblk = items
        carry = update(carry, kblk, vblk, pblk, dblk)
        return (carry, None)

    state, unused = lax.scan(
        one_step, state, (kparts, vparts, kpos.reshape(steps, width), kdoc.reshape(steps, width))
    )
    largest, total, summed = state
    attended = (summed / jnp.transpose(total, (2, 0, 1))[..., None]).astype(jnp.bfloat16)
    attended = attended.reshape(tok_rows, local_heads * DH)
    partial_out = jnp.dot(
        attended,
        lax.all_gather(out_weight, "seq", axis=1, tiled=True),
        preferred_element_type=jnp.float32,
    )
    return lax.psum_scatter(
        partial_out.astype(jnp.bfloat16), "head", scatter_dimension=1, tiled=True
    )


def solution(mesh):
    n, heads = mesh.shape["seq"], mesh.shape["head"]

    def on_each(queries, keys, values, doc_ids, span_order, out_weight):
        span = queries.shape[0] // 2
        ring = (
            4 <= n <= 16
            and n % 2 == 0
            and n % heads == 0
            and heads & (heads - 1) == 0
            and keys.shape[1] == DH
            and span % LANES == 0
            and out_weight.shape[1] % (2 * LANES) == 0
        )
        args = (queries, keys, values, doc_ids, span_order, out_weight)
        return ring_device(n, heads, *args) if ring else on_device(*args)

    return jax.shard_map(
        on_each,
        mesh=mesh,
        in_specs=(P("seq", "head"), P("seq", "head"), P("seq", "head"), P(), P(), P("head", "seq")),
        out_specs=P("seq", "head"),
        check_vma=False,
    )
```

```python
import functools
import math

import jax
import jax.numpy as jnp
from jax import lax
from jax.experimental import pallas as pl
from jax.experimental.pallas import tpu as pltpu
from jax.sharding import PartitionSpec as P

DH = 128
LANES = 128
NONE = -1000
VMEM = pl.BlockSpec(memory_space=pltpu.VMEM)
SMEM = pl.BlockSpec(memory_space=pltpu.SMEM)


def ring_order(n):
    return list(range(0, n, 2)) + list(range(n - 1, 0, -2))


def ring_tables(n):
    ring = ring_order(n)
    place = {s: i for i, s in enumerate(ring)}
    forward = [(ring[i], ring[(i + 1) % n]) for i in range(n)]
    backward = [(b, a) for a, b in forward]
    sources = []
    for s in range(n):
        row = [s]
        for hop in range(1, n // 2):
            row.append(ring[(place[s] - hop) % n])
            row.append(ring[(place[s] + hop) % n])
        row.append(ring[(place[s] + n // 2) % n])
        sources.append(row)
    return forward, backward, sources


def attention_kernel(
    n, span, group, src_ref, order_ref, first_ref, docs_ref, q_ref, *rest
):
    kv_refs, (out_ref, s_ref, m_ref, l_ref, acc_ref) = rest[:n], rest[n:]
    base2 = math.log2(math.e) / math.sqrt(DH)
    mine = lax.axis_index("seq")
    dims = (((1,), (1,)), ((), ()))

    for part in range(2):
        rows = pl.ds(part * span, span)
        qpos = order_ref[2 * mine + part]
        q = jnp.concatenate(
            [q_ref[rows, h * DH : (h + 1) * DH] for h in range(group)], axis=0
        )
        qdoc = jnp.transpose(
            jnp.broadcast_to(docs_ref[pl.ds(qpos, 1), :], (span, span)).astype(jnp.float32)
        )
        qfirst = first_ref[qpos * span]
        ahead = lax.broadcasted_iota(jnp.int32, (span, span), 1) - lax.broadcasted_iota(
            jnp.int32, (span, span), 0
        )
        m_ref[...] = jnp.full_like(m_ref, -1e30)
        l_ref[...] = jnp.zeros_like(l_ref)
        acc_ref[...] = jnp.zeros_like(acc_ref)

        def seen(j):
            kpos = order_ref[2 * src_ref[mine * n + j // 2] + j % 2]
            return kpos, (kpos <= qpos) & (first_ref[kpos * span + span - 1] >= qfirst)

        for j in range(2 * n):
            kpos, live = seen(j)

            @pl.when(live)
            def _():
                k = kv_refs[j // 2][(j % 2) * span : (j % 2 + 1) * span, :DH]
                s = lax.dot_general(q, k, dims, preferred_element_type=jnp.float32)
                kdoc = docs_ref[pl.ds(kpos, 1), :].astype(jnp.float32)
                visible = (qdoc == kdoc) & (ahead <= (qpos - kpos) * span)
                s = jnp.where(visible[None], s.reshape(group, span, span), -1e30)
                s = s.reshape(group * span, span)
                s_ref[:, j * span : (j + 1) * span] = s
                m_ref[...] = jnp.maximum(m_ref[...], s)

        largest = jnp.max(m_ref[...], axis=1, keepdims=True) * base2

        for j in range(2 * n):
            kpos, live = seen(j)

            @pl.when(live)
            def _():
                p = jnp.exp2(s_ref[:, j * span : (j + 1) * span] * base2 - largest)
                l_ref[...] += p
                v = kv_refs[j // 2][(j % 2) * span : (j % 2 + 1) * span, DH:]
                acc_ref[...] += jnp.dot(
                    p.astype(jnp.bfloat16), v, preferred_element_type=jnp.float32
                )

        total = jnp.sum(l_ref[...], axis=1, keepdims=True)
        attended = (acc_ref[...] / total).astype(jnp.bfloat16)
        for h in range(group):
            out_ref[rows, h * DH : (h + 1) * DH] = attended[h * span : (h + 1) * span]


def project_kernel(blocks, stride, tab_ref, a_ref, *rest):
    w_refs, (send_ref, keep_ref) = rest[:-2], rest[-2:]
    s, h = lax.axis_index("seq"), lax.axis_index("head")
    a = a_ref[...]
    split = len(w_refs) // blocks
    for b in range(blocks):
        at = tab_ref[s * stride[0] + h * stride[1] + b]
        for i in range(split):
            w = w_refs[b * split + i][...]
            c = jnp.dot(a, w, preferred_element_type=jnp.float32).astype(jnp.bfloat16)
            cols = slice(i * w.shape[1], (i + 1) * w.shape[1])

            @pl.when(at >= 0)
            def _():
                send_ref[jnp.maximum(at, 0), :, cols] = c

            @pl.when(at < 0)
            def _():
                keep_ref[jnp.maximum(-1 - at, 0), :, cols] = c


def fold_kernel(blocks, stride, tab_ref, kept_ref, came_ref, send_ref, keep_ref):
    s, h = lax.axis_index("seq"), lax.axis_index("head")
    for b in range(blocks):
        at = tab_ref[s * stride[0] + h * stride[1] + b]

        @pl.when(at != NONE)
        def _():
            c = kept_ref[b].astype(jnp.float32) + came_ref[b].astype(jnp.float32)
            c = c.astype(jnp.bfloat16)

            @pl.when(at >= 0)
            def _():
                send_ref[jnp.maximum(at, 0)] = c

            @pl.when(at < 0)
            def _():
                keep_ref[jnp.maximum(-1 - at, 0)] = c


def finish_kernel(counts, stride, tab_ref, *rest):
    kept, came, out_ref = rest[: len(counts)], rest[len(counts) : -1], rest[-1]
    s, h = lax.axis_index("seq"), lax.axis_index("head")
    col = 0
    for r, count in enumerate(counts):
        for b in range(count):
            half = tab_ref[s * stride[0] + h * stride[1] + col]
            col += 1

            @pl.when(half != NONE)
            def _():
                width = kept[r].shape[2]
                c = kept[r][b].astype(jnp.float32) + came[r][b].astype(jnp.float32)
                start = pl.multiple_of(jnp.maximum(half, 0) * width, LANES)
                out_ref[:, pl.ds(start, width)] = c.astype(out_ref.dtype)


def reduce_plan(n, heads, sources, rounds):
    per = n // heads
    plan = []
    for places in rounds:
        held = {(s, h): [sources[s][p] for p in places] for s in range(n) for h in range(heads)}
        stages = []
        step = 1
        while step < heads:
            table, pairs = {}, []
            sends, keeps = {}, {}
            for (s, h), blocks in held.items():
                sent = [b for b in blocks if (b // per ^ h) & step]
                kept = [b for b in blocks if not (b // per ^ h) & step]
                table[s, h] = [
                    sent.index(b) if (b // per ^ h) & step else -1 - kept.index(b) for b in blocks
                ]
                sends[s, h], keeps[s, h] = sent, kept
                if sent:
                    pairs.append((s * heads + h, s * heads + (h ^ step)))
            n_send = max(1, max(len(v) for v in sends.values()))
            n_keep = max(n_send, max(len(v) for v in keeps.values()))
            stages.append((table, pairs, n_send, n_keep))
            held = keeps
            step *= 2
        plan.append((stages, held))
    return plan


def as_table(n, heads, rows, length):
    flat = []
    for s in range(n):
        for h in range(heads):
            row = list(rows[s, h])
            flat += row + [NONE] * (length - len(row))
    return jnp.asarray(flat, jnp.int32), (heads * length, length)


def ring_device(n, heads, queries, keys, values, doc_ids, span_order, out_weight):
    tok_rows = queries.shape[0]
    span = tok_rows // 2
    group = queries.shape[1] // DH
    width = out_weight.shape[1]
    per = n // heads
    forward, backward, sources = ring_tables(n)

    def gather(pieces):
        ups, downs = list(pieces), list(pieces)
        late = (len(pieces) + 1) // 2
        got = [list(pieces)]
        for hop in range(1, n // 2 + 1):
            last = hop == n // 2
            for i in range(len(pieces)):
                if not last or i < late:
                    ups[i] = lax.ppermute(ups[i], "seq", forward)
                if not last or i >= late:
                    downs[i] = lax.ppermute(downs[i], "seq", backward)
            if last:
                got.append(ups[:late] + downs[late:])
            else:
                got.append(list(ups))
                got.append(list(downs))
        return got

    both = jnp.concatenate([keys, values], axis=1)
    kv = [g[0] for g in gather([both])]
    split = 2
    out_weight, both = lax.optimization_barrier((out_weight, both))
    w = gather([out_weight[:, i * width // split : (i + 1) * width // split] for i in range(split)])

    table = jnp.asarray([p for row in sources for p in row], jnp.int32)
    attended = pl.pallas_call(
        functools.partial(attention_kernel, n, span, group),
        out_shape=jax.ShapeDtypeStruct((tok_rows, group * DH), jnp.bfloat16),
        in_specs=[SMEM, SMEM, SMEM] + [VMEM] * (2 + n),
        out_specs=VMEM,
        scratch_shapes=[
            pltpu.VMEM((group * span, 2 * n * span), jnp.float32),
            pltpu.VMEM((group * span, span), jnp.float32),
            pltpu.VMEM((group * span, span), jnp.float32),
            pltpu.VMEM((group * span, DH), jnp.float32),
        ],
        cost_estimate=pl.CostEstimate(
            flops=4 * group * tok_rows * n * tok_rows * DH,
            bytes_accessed=n * tok_rows * 4 * DH,
            transcendentals=group * tok_rows * n * tok_rows,
        ),
        name="attention",
    )(table, span_order, doc_ids, doc_ids.reshape(-1, span), queries, *kv)

    def block(count):
        return jax.ShapeDtypeStruct((count, tok_rows, width), jnp.bfloat16)

    rounds = [list(range(n - 3)), [n - 3, n - 2], [n - 1]]
    kepts, cames, counts, halves = [], [], [], {}
    for places, (stages, held) in zip(rounds, reduce_plan(n, heads, sources, rounds)):
        for i, (rows, pairs, n_send, n_keep) in enumerate(stages):
            if i == 0:
                tab, stride = as_table(n, heads, rows, len(places))
                pieces = [piece for p in places for piece in w[p]]
                send, keep = pl.pallas_call(
                    functools.partial(project_kernel, len(places), stride),
                    out_shape=(block(n_send), block(n_keep)),
                    in_specs=[SMEM] + [VMEM] * (1 + len(pieces)),
                    out_specs=(VMEM, VMEM),
                    cost_estimate=pl.CostEstimate(
                        flops=2 * tok_rows * group * DH * width * len(places),
                        bytes_accessed=2 * group * DH * width * len(places),
                        transcendentals=0,
                    ),
                    name="project",
                )(tab, attended, *pieces)
            else:
                tab, stride = as_table(n, heads, rows, keep.shape[0])
                send, keep = pl.pallas_call(
                    functools.partial(fold_kernel, came.shape[0], stride),
                    out_shape=(block(n_send), block(n_keep)),
                    in_specs=[SMEM, VMEM, VMEM],
                    out_specs=(VMEM, VMEM),
                    cost_estimate=pl.CostEstimate(
                        flops=tok_rows * width * came.shape[0],
                        bytes_accessed=8 * tok_rows * width * came.shape[0],
                        transcendentals=0,
                    ),
                    name="fold",
                )(tab, keep, came)
            came = lax.ppermute(send, ("seq", "head"), pairs)
        kepts.append(keep)
        cames.append(came)
        counts.append(came.shape[0])
        for key, blocks in held.items():
            row = [b % per for b in blocks]
            halves.setdefault(key, []).extend(row + [NONE] * (came.shape[0] - len(row)))

    tab, stride = as_table(n, heads, halves, sum(counts))
    return pl.pallas_call(
        functools.partial(finish_kernel, counts, stride),
        out_shape=jax.ShapeDtypeStruct((tok_rows, per * width), jnp.bfloat16),
        in_specs=[SMEM] + [VMEM] * (2 * len(counts)),
        out_specs=VMEM,
        name="finish",
    )(tab, *kepts, *cames)


def on_device(queries, keys, values, doc_ids, span_order, out_weight):
    tok_rows = queries.shape[0]
    span = tok_rows // 2
    local_heads = queries.shape[1] // DH
    local_kv = keys.shape[1] // DH
    group_size = local_heads // local_kv
    n_blocks = span_order.shape[0]
    scale = 1.0 / math.sqrt(DH)
    mine = lax.axis_index("seq")
    own_blocks = lax.dynamic_slice_in_dim(span_order, 2 * mine, 2, 0)
    local_rows = jnp.arange(tok_rows, dtype=jnp.int32)
    qpos = jnp.where(local_rows < span, own_blocks[0], own_blocks[1]) * span + local_rows % span
    qdoc = jnp.take(doc_ids, qpos)
    q_heads = queries.reshape(tok_rows, local_kv, group_size, DH)

    def update(state, kblk, vblk, kpos, kdoc):
        largest, total, summed = state
        count = kblk.shape[0]
        k_heads = kblk.reshape(count, local_kv, DH)
        v_heads = vblk.reshape(count, local_kv, DH)
        scores = (
            jnp.einsum("qhgd,khd->hgqk", q_heads, k_heads, preferred_element_type=jnp.float32)
            * scale
        )
        visible = (qdoc[:, None] == kdoc[None, :]) & (kpos[None, :] <= qpos[:, None])
        masked = jnp.where(visible, scores, jnp.float32(-1e30))
        new_largest = jnp.maximum(largest, jnp.max(masked, axis=-1))
        factor = jnp.exp(largest - new_largest)
        weights = jnp.where(visible, jnp.exp(masked - new_largest[..., None]), jnp.float32(0.0))
        total = total * factor + jnp.sum(weights, axis=-1)
        weights_b = weights.astype(jnp.bfloat16)
        added = jnp.einsum("hgqk,khd->qhgd", weights_b, v_heads, preferred_element_type=jnp.float32)
        summed = summed * jnp.transpose(factor, (2, 0, 1))[..., None] + added
        return (new_largest, total, summed)

    initial = (
        jnp.full((local_kv, group_size, tok_rows), -1e30, jnp.float32),
        jnp.zeros((local_kv, group_size, tok_rows), jnp.float32),
        jnp.zeros((tok_rows, local_kv, group_size, DH), jnp.float32),
    )
    state = initial
    kpiece = lax.all_gather(keys, "seq", axis=0, tiled=True)
    vpiece = lax.all_gather(values, "seq", axis=0, tiled=True)
    count = kpiece.shape[0]
    width = math.gcd(count, 1024)
    steps = count // width
    rows = jnp.arange(count, dtype=jnp.int32)
    match = (rows // span)[:, None] == jnp.arange(n_blocks, dtype=jnp.int32)[None, :]
    owner = jnp.sum(jnp.where(match, span_order[None, :], 0), axis=1)
    kpos = owner * span + rows % span
    kdoc = jnp.take(doc_ids, kpos)
    kparts = kpiece.reshape(steps, width, kpiece.shape[1])
    vparts = vpiece.reshape(steps, width, vpiece.shape[1])

    def one_step(carry, items):
        kblk, vblk, pblk, dblk = items
        carry = update(carry, kblk, vblk, pblk, dblk)
        return (carry, None)

    state, unused = lax.scan(
        one_step, state, (kparts, vparts, kpos.reshape(steps, width), kdoc.reshape(steps, width))
    )
    largest, total, summed = state
    attended = (summed / jnp.transpose(total, (2, 0, 1))[..., None]).astype(jnp.bfloat16)
    attended = attended.reshape(tok_rows, local_heads * DH)
    partial_out = jnp.dot(
        attended,
        lax.all_gather(out_weight, "seq", axis=1, tiled=True),
        preferred_element_type=jnp.float32,
    )
    return lax.psum_scatter(
        partial_out.astype(jnp.bfloat16), "head", scatter_dimension=1, tiled=True
    )


def solution(mesh):
    n, heads = mesh.shape["seq"], mesh.shape["head"]

    def on_each(queries, keys, values, doc_ids, span_order, out_weight):
        span = queries.shape[0] // 2
        ring = (
            4 <= n <= 16
            and n % 2 == 0
            and n % heads == 0
            and heads & (heads - 1) == 0
            and keys.shape[1] == DH
            and span % LANES == 0
            and out_weight.shape[1] % (2 * LANES) == 0
        )
        args = (queries, keys, values, doc_ids, span_order, out_weight)
        return ring_device(n, heads, *args) if ring else on_device(*args)

    return jax.shard_map(
        on_each,
        mesh=mesh,
        in_specs=(P("seq", "head"), P("seq", "head"), P("seq", "head"), P(), P(), P("head", "seq")),
        out_specs=P("seq", "head"),
        check_vma=False,
    )
```

```python
import functools
import math

import jax
import jax.numpy as jnp
from jax import lax
from jax.experimental import pallas as pl
from jax.experimental.pallas import tpu as pltpu
from jax.sharding import PartitionSpec as P


DH = 128
LANES = 128
NONE = -1000
VMEM = pl.BlockSpec(memory_space=pltpu.VMEM)
SMEM = pl.BlockSpec(memory_space=pltpu.SMEM)


def ring_order(n):
    return list(range(0, n, 2)) + list(range(n - 1, 0, -2))


def ring_tables(n):
    ring = ring_order(n)
    place = {s: i for i, s in enumerate(ring)}
    forward = [(ring[i], ring[(i + 1) % n]) for i in range(n)]
    backward = [(b, a) for a, b in forward]
    sources = []
    for s in range(n):
        row = [s]
        for hop in range(1, n // 2):
            row.append(ring[(place[s] - hop) % n])
            row.append(ring[(place[s] + hop) % n])
        row.append(ring[(place[s] + n // 2) % n])
        sources.append(row)
    return forward, backward, sources


def attention_kernel(
    n, span, group, src_ref, order_ref, first_ref, docs_ref, q_ref, *rest
):
    kv_refs, (out_ref, s_ref, m_ref, l_ref, acc_ref) = rest[:n], rest[n:]
    base2 = math.log2(math.e) / math.sqrt(DH)
    mine = lax.axis_index("seq")
    dims = (((1,), (1,)), ((), ()))

    for part in range(2):
        rows = pl.ds(part * span, span)
        qpos = order_ref[2 * mine + part]
        q = jnp.concatenate(
            [q_ref[rows, h * DH : (h + 1) * DH] for h in range(group)], axis=0
        )
        qdoc = jnp.transpose(
            jnp.broadcast_to(docs_ref[pl.ds(qpos, 1), :], (span, span)).astype(jnp.float32)
        )
        qfirst = first_ref[qpos * span]
        ahead = lax.broadcasted_iota(jnp.int32, (span, span), 1) - lax.broadcasted_iota(
            jnp.int32, (span, span), 0
        )
        m_ref[...] = jnp.full_like(m_ref, -1e30)
        l_ref[...] = jnp.zeros_like(l_ref)
        acc_ref[...] = jnp.zeros_like(acc_ref)

        def seen(j):
            kpos = order_ref[2 * src_ref[mine * n + j // 2] + j % 2]
            return kpos, (kpos <= qpos) & (first_ref[kpos * span + span - 1] >= qfirst)

        for j in range(2 * n):
            kpos, live = seen(j)

            @pl.when(live)
            def _():
                k = kv_refs[j // 2][(j % 2) * span : (j % 2 + 1) * span, :DH]
                s = lax.dot_general(q, k, dims, preferred_element_type=jnp.float32)
                kdoc = docs_ref[pl.ds(kpos, 1), :].astype(jnp.float32)
                visible = (qdoc == kdoc) & (ahead <= (qpos - kpos) * span)
                s = jnp.where(visible[None], s.reshape(group, span, span), -1e30)
                s = s.reshape(group * span, span)
                s_ref[:, j * span : (j + 1) * span] = s
                m_ref[...] = jnp.maximum(m_ref[...], s)

        largest = jnp.max(m_ref[...], axis=1, keepdims=True) * base2

        for j in range(2 * n):
            kpos, live = seen(j)

            @pl.when(live)
            def _():
                p = jnp.exp2(s_ref[:, j * span : (j + 1) * span] * base2 - largest)
                l_ref[...] += p
                v = kv_refs[j // 2][(j % 2) * span : (j % 2 + 1) * span, DH:]
                acc_ref[...] += jnp.dot(
                    p.astype(jnp.bfloat16), v, preferred_element_type=jnp.float32
                )

        total = jnp.sum(l_ref[...], axis=1, keepdims=True)
        attended = (acc_ref[...] / total).astype(jnp.bfloat16)
        for h in range(group):
            out_ref[rows, h * DH : (h + 1) * DH] = attended[h * span : (h + 1) * span]


def project_kernel(blocks, stride, tab_ref, a_ref, *rest):
    w_refs, (send_ref, keep_ref) = rest[:-2], rest[-2:]
    s, h = lax.axis_index("seq"), lax.axis_index("head")
    a = a_ref[...]
    split = len(w_refs) // blocks
    for b in range(blocks):
        at = tab_ref[s * stride[0] + h * stride[1] + b]
        for i in range(split):
            w = w_refs[b * split + i][...]
            c = jnp.dot(a, w, preferred_element_type=jnp.float32).astype(jnp.bfloat16)
            cols = slice(i * w.shape[1], (i + 1) * w.shape[1])

            @pl.when(at >= 0)
            def _():
                send_ref[jnp.maximum(at, 0), :, cols] = c

            @pl.when(at < 0)
            def _():
                keep_ref[jnp.maximum(-1 - at, 0), :, cols] = c


def fold_kernel(blocks, stride, tab_ref, kept_ref, came_ref, send_ref, keep_ref):
    s, h = lax.axis_index("seq"), lax.axis_index("head")
    for b in range(blocks):
        at = tab_ref[s * stride[0] + h * stride[1] + b]

        @pl.when(at != NONE)
        def _():
            c = kept_ref[b].astype(jnp.float32) + came_ref[b].astype(jnp.float32)
            c = c.astype(jnp.bfloat16)

            @pl.when(at >= 0)
            def _():
                send_ref[jnp.maximum(at, 0)] = c

            @pl.when(at < 0)
            def _():
                keep_ref[jnp.maximum(-1 - at, 0)] = c


def finish_kernel(counts, stride, tab_ref, *rest):
    kept, came, out_ref = rest[: len(counts)], rest[len(counts) : -1], rest[-1]
    s, h = lax.axis_index("seq"), lax.axis_index("head")
    col = 0
    for r, count in enumerate(counts):
        for b in range(count):
            half = tab_ref[s * stride[0] + h * stride[1] + col]
            col += 1

            @pl.when(half != NONE)
            def _():
                width = kept[r].shape[2]
                c = kept[r][b].astype(jnp.float32) + came[r][b].astype(jnp.float32)
                start = pl.multiple_of(jnp.maximum(half, 0) * width, LANES)
                out_ref[:, pl.ds(start, width)] = c.astype(out_ref.dtype)


def reduce_plan(n, heads, sources, rounds):
    per = n // heads
    plan = []
    for places in rounds:
        held = {(s, h): [sources[s][p] for p in places] for s in range(n) for h in range(heads)}
        stages = []
        step = 1
        while step < heads:
            table, pairs = {}, []
            sends, keeps = {}, {}
            for (s, h), blocks in held.items():
                sent = [b for b in blocks if (b // per ^ h) & step]
                kept = [b for b in blocks if not (b // per ^ h) & step]
                table[s, h] = [
                    sent.index(b) if (b // per ^ h) & step else -1 - kept.index(b) for b in blocks
                ]
                sends[s, h], keeps[s, h] = sent, kept
                if sent:
                    pairs.append((s * heads + h, s * heads + (h ^ step)))
            n_send = max(1, max(len(v) for v in sends.values()))
            n_keep = max(n_send, max(len(v) for v in keeps.values()))
            stages.append((table, pairs, n_send, n_keep))
            held = keeps
            step *= 2
        plan.append((stages, held))
    return plan


def as_table(n, heads, rows, length):
    flat = []
    for s in range(n):
        for h in range(heads):
            row = list(rows[s, h])
            flat += row + [NONE] * (length - len(row))
    return jnp.asarray(flat, jnp.int32), (heads * length, length)


def ring_device(n, heads, queries, keys, values, doc_ids, span_order, out_weight):
    tok_rows = queries.shape[0]
    span = tok_rows // 2
    group = queries.shape[1] // DH
    width = out_weight.shape[1]
    per = n // heads
    forward, backward, sources = ring_tables(n)

    def gather(pieces):
        def move(x, pairs):
            return lax.ppermute(x, "seq", pairs)

        ups, downs = list(pieces), list(pieces)
        late = (len(pieces) + 1) // 2
        got = [list(pieces)]
        for hop in range(1, n // 2 + 1):
            last = hop == n // 2
            for i in range(len(pieces)):
                if not last or i < late:
                    ups[i] = move(ups[i], forward)
                if not last or i >= late:
                    downs[i] = move(downs[i], backward)
            if last:
                got.append(ups[:late] + downs[late:])
            else:
                got.append(list(ups))
                got.append(list(downs))
        return got

    both = jnp.concatenate([keys, values], axis=1)
    kv = [g[0] for g in gather([both])]
    split = 2
    out_weight, both = lax.optimization_barrier((out_weight, both))
    w = gather([out_weight[:, i * width // split : (i + 1) * width // split] for i in range(split)])

    table = jnp.asarray([p for row in sources for p in row], jnp.int32)
    attended = pl.pallas_call(
        functools.partial(attention_kernel, n, span, group),
        out_shape=jax.ShapeDtypeStruct((tok_rows, group * DH), jnp.bfloat16),
        in_specs=[SMEM, SMEM, SMEM] + [VMEM] * (2 + n),
        out_specs=VMEM,
        scratch_shapes=[
            pltpu.VMEM((group * span, 2 * n * span), jnp.float32),
            pltpu.VMEM((group * span, span), jnp.float32),
            pltpu.VMEM((group * span, span), jnp.float32),
            pltpu.VMEM((group * span, DH), jnp.float32),
        ],
        cost_estimate=pl.CostEstimate(
            flops=4 * group * tok_rows * n * tok_rows * DH,
            bytes_accessed=n * tok_rows * 4 * DH,
            transcendentals=group * tok_rows * n * tok_rows,
        ),
        compiler_params=pltpu.CompilerParams(vmem_limit_bytes=16 * 2**20),
        name="attention",
    )(table, span_order, doc_ids, doc_ids.reshape(-1, span), queries, *kv)

    def block(count):
        return jax.ShapeDtypeStruct((count, tok_rows, width), jnp.bfloat16)

    rounds = [list(range(n - 3)), [n - 3, n - 2], [n - 1]]
    kepts, cames, counts, halves = [], [], [], {}
    for places, (stages, held) in zip(rounds, reduce_plan(n, heads, sources, rounds)):
        for i, (rows, pairs, n_send, n_keep) in enumerate(stages):
            if i == 0:
                tab, stride = as_table(n, heads, rows, len(places))
                pieces = [piece for p in places for piece in w[p]]
                kernel = pl.pallas_call(
                    functools.partial(project_kernel, len(places), stride),
                    out_shape=(block(n_send), block(n_keep)),
                    in_specs=[SMEM] + [VMEM] * (1 + len(pieces)),
                    out_specs=(VMEM, VMEM),
                    cost_estimate=pl.CostEstimate(
                        flops=2 * tok_rows * group * DH * width * len(places),
                        bytes_accessed=2 * group * DH * width * len(places),
                        transcendentals=0,
                    ),
                    compiler_params=pltpu.CompilerParams(vmem_limit_bytes=8 * 2**20),
                    name="project",
                )
                send, keep = kernel(tab, attended, *pieces)
            else:
                tab, stride = as_table(n, heads, rows, keep.shape[0])
                send, keep = pl.pallas_call(
                    functools.partial(fold_kernel, came.shape[0], stride),
                    out_shape=(block(n_send), block(n_keep)),
                    in_specs=[SMEM, VMEM, VMEM],
                    out_specs=(VMEM, VMEM),
                    cost_estimate=pl.CostEstimate(
                        flops=tok_rows * width * came.shape[0],
                        bytes_accessed=8 * tok_rows * width * came.shape[0],
                        transcendentals=0,
                    ),
                    compiler_params=pltpu.CompilerParams(vmem_limit_bytes=8 * 2**20),
                    name="fold",
                )(tab, keep, came)
            came = lax.ppermute(send, ("seq", "head"), pairs)
        kepts.append(keep)
        cames.append(came)
        counts.append(came.shape[0])
        for key, blocks in held.items():
            row = [b % per for b in blocks]
            halves.setdefault(key, []).extend(row + [NONE] * (came.shape[0] - len(row)))

    tab, stride = as_table(n, heads, halves, sum(counts))
    return pl.pallas_call(
        functools.partial(finish_kernel, counts, stride),
        out_shape=jax.ShapeDtypeStruct((tok_rows, per * width), jnp.bfloat16),
        in_specs=[SMEM] + [VMEM] * (2 * len(counts)),
        out_specs=VMEM,
        compiler_params=pltpu.CompilerParams(vmem_limit_bytes=8 * 2**20),
                    name="finish",
    )(tab, *kepts, *cames)


def on_device(queries, keys, values, doc_ids, span_order, out_weight):
    tok_rows = queries.shape[0]
    span = tok_rows // 2
    local_heads = queries.shape[1] // DH
    local_kv = keys.shape[1] // DH
    group_size = local_heads // local_kv
    n_blocks = span_order.shape[0]
    scale = 1.0 / math.sqrt(DH)
    mine = lax.axis_index("seq")
    own_blocks = lax.dynamic_slice_in_dim(span_order, 2 * mine, 2, 0)
    local_rows = jnp.arange(tok_rows, dtype=jnp.int32)
    qpos = jnp.where(local_rows < span, own_blocks[0], own_blocks[1]) * span + local_rows % span
    qdoc = jnp.take(doc_ids, qpos)
    q_heads = queries.reshape(tok_rows, local_kv, group_size, DH)

    def update(state, kblk, vblk, kpos, kdoc):
        largest, total, summed = state
        count = kblk.shape[0]
        k_heads = kblk.reshape(count, local_kv, DH)
        v_heads = vblk.reshape(count, local_kv, DH)
        scores = (
            jnp.einsum("qhgd,khd->hgqk", q_heads, k_heads, preferred_element_type=jnp.float32)
            * scale
        )
        visible = (qdoc[:, None] == kdoc[None, :]) & (kpos[None, :] <= qpos[:, None])
        masked = jnp.where(visible, scores, jnp.float32(-1e30))
        new_largest = jnp.maximum(largest, jnp.max(masked, axis=-1))
        factor = jnp.exp(largest - new_largest)
        weights = jnp.where(visible, jnp.exp(masked - new_largest[..., None]), jnp.float32(0.0))
        total = total * factor + jnp.sum(weights, axis=-1)
        weights_b = weights.astype(jnp.bfloat16)
        added = jnp.einsum("hgqk,khd->qhgd", weights_b, v_heads, preferred_element_type=jnp.float32)
        summed = summed * jnp.transpose(factor, (2, 0, 1))[..., None] + added
        return (new_largest, total, summed)

    initial = (
        jnp.full((local_kv, group_size, tok_rows), -1e30, jnp.float32),
        jnp.zeros((local_kv, group_size, tok_rows), jnp.float32),
        jnp.zeros((tok_rows, local_kv, group_size, DH), jnp.float32),
    )
    state = initial
    kpiece = lax.all_gather(keys, "seq", axis=0, tiled=True)
    vpiece = lax.all_gather(values, "seq", axis=0, tiled=True)
    count = kpiece.shape[0]
    width = math.gcd(count, 1024)
    steps = count // width
    rows = jnp.arange(count, dtype=jnp.int32)
    match = (rows // span)[:, None] == jnp.arange(n_blocks, dtype=jnp.int32)[None, :]
    owner = jnp.sum(jnp.where(match, span_order[None, :], 0), axis=1)
    kpos = owner * span + rows % span
    kdoc = jnp.take(doc_ids, kpos)
    kparts = kpiece.reshape(steps, width, kpiece.shape[1])
    vparts = vpiece.reshape(steps, width, vpiece.shape[1])

    def one_step(carry, items):
        kblk, vblk, pblk, dblk = items
        carry = update(carry, kblk, vblk, pblk, dblk)
        return (carry, None)

    state, _ = lax.scan(
        one_step, state, (kparts, vparts, kpos.reshape(steps, width), kdoc.reshape(steps, width))
    )
    _, total, summed = state
    attended = (summed / jnp.transpose(total, (2, 0, 1))[..., None]).astype(jnp.bfloat16)
    attended = attended.reshape(tok_rows, local_heads * DH)
    partial_out = jnp.dot(
        attended,
        lax.all_gather(out_weight, "seq", axis=1, tiled=True),
        preferred_element_type=jnp.float32,
    )
    return lax.psum_scatter(
        partial_out.astype(jnp.bfloat16), "head", scatter_dimension=1, tiled=True
    )


def solution(mesh):
    n, heads = mesh.shape["seq"], mesh.shape["head"]

    def on_each(queries, keys, values, doc_ids, span_order, out_weight):
        span = queries.shape[0] // 2
        ring = (
            4 <= n <= 16
            and n % 2 == 0
            and n % heads == 0
            and heads & (heads - 1) == 0
            and keys.shape[1] == DH
            and span % LANES == 0
            and out_weight.shape[1] % (2 * LANES) == 0
        )
        args = (queries, keys, values, doc_ids, span_order, out_weight)
        if not ring:
            return on_device(*args)
        return ring_device(n, heads, *args)

    return jax.shard_map(
        on_each,
        mesh=mesh,
        in_specs=(P("seq", "head"), P("seq", "head"), P("seq", "head"), P(), P(), P("head", "seq")),
        out_specs=P("seq", "head"),
        check_vma=False,
    )
```

```python
import functools
import math

import jax
import jax.numpy as jnp
from jax import lax
from jax.experimental import pallas as pl
from jax.experimental.pallas import tpu as pltpu
from jax.sharding import PartitionSpec as P


DH = 128
LANES = 128
NONE = -1000
VMEM = pl.BlockSpec(memory_space=pltpu.VMEM)
SMEM = pl.BlockSpec(memory_space=pltpu.SMEM)
NONE = 15


def limit(mib):
    return pltpu.CompilerParams(vmem_limit_bytes=mib * 2**20)


def lookup(values, index):
    words = []
    for i in range(0, len(values), 8):
        word = sum(v << 4 * k for k, v in enumerate(values[i : i + 8]))
        words.append(word - 2**32 if word >= 2**31 else word)
    word = jnp.int32(words[0])
    for i in range(1, len(words)):
        word = jnp.where(index // 8 == i, jnp.int32(words[i]), word)
    return (word >> (4 * (index % 8))) & 15


def ring_order(n):
    return list(range(0, n, 2)) + list(range(n - 1, 0, -2))


def attention_kernel(n, span, group, sources, order_ref, docid_ref, docs_ref, q_ref, *rest):
    kv_refs, (out_ref, s_ref, m_ref, l_ref, acc_ref) = rest[:n], rest[n:]
    base2 = math.log2(math.e) / math.sqrt(DH)
    mine = lax.axis_index("seq")
    dims = (((1,), (1,)), ((), ()))
    kposs = []
    for i in range(n):
        source = lookup([row[i] for row in sources], mine)
        kposs += [order_ref[2 * source], order_ref[2 * source + 1]]

    for part in range(2):
        rows = pl.ds(part * span, span)
        qpos = order_ref[2 * mine + part]
        q = jnp.concatenate(
            [q_ref[rows, h * DH : (h + 1) * DH] for h in range(group)], axis=0
        )
        qdoc = jnp.transpose(
            jnp.broadcast_to(docs_ref[pl.ds(qpos, 1), :], (span, span)).astype(jnp.float32)
        )
        qfirst = docid_ref[qpos * span]
        ahead = lax.broadcasted_iota(jnp.int32, (span, span), 1) - lax.broadcasted_iota(
            jnp.int32, (span, span), 0
        )
        m_ref[...] = jnp.full_like(m_ref, -1e30)
        l_ref[...] = jnp.zeros_like(l_ref)
        acc_ref[...] = jnp.zeros_like(acc_ref)
        lives = [(k <= qpos) & (docid_ref[k * span + span - 1] >= qfirst) for k in kposs]

        for j in range(2 * n):

            @pl.when(lives[j])
            def _():
                k = kv_refs[j // 2][(j % 2) * span : (j % 2 + 1) * span, :DH]
                s = lax.dot_general(q, k, dims, preferred_element_type=jnp.float32)
                kdoc = docs_ref[pl.ds(kposs[j], 1), :].astype(jnp.float32)
                visible = (qdoc == kdoc) & (ahead <= (qpos - kposs[j]) * span)
                s = jnp.where(visible[None], s.reshape(group, span, span), -1e30)
                s = s.reshape(group * span, span)
                s_ref[:, j * span : (j + 1) * span] = s
                m_ref[...] = jnp.maximum(m_ref[...], s)

        largest = jnp.max(m_ref[...], axis=1, keepdims=True) * base2

        for j in range(2 * n):

            @pl.when(lives[j])
            def _():
                p = jnp.exp2(s_ref[:, j * span : (j + 1) * span] * base2 - largest)
                l_ref[...] += p
                v = kv_refs[j // 2][(j % 2) * span : (j % 2 + 1) * span, DH:]
                acc_ref[...] += jnp.dot(
                    p.astype(jnp.bfloat16), v, preferred_element_type=jnp.float32
                )

        total = jnp.sum(l_ref[...], axis=1, keepdims=True)
        attended = (acc_ref[...] / total).astype(jnp.bfloat16)
        for h in range(group):
            out_ref[rows, h * DH : (h + 1) * DH] = attended[h * span : (h + 1) * span]


def place():
    return lax.axis_index("seq") * lax.axis_size("head") + lax.axis_index("head")


def project_kernel(codes, per, a_ref, b_ref, *rest):
    w_refs, out_refs = rest[: 2 * len(codes)], rest[2 * len(codes) :]
    me = place()
    for i, values in enumerate(codes):
        at = lookup(values, me)
        c = jnp.dot(a_ref[...], w_refs[2 * i][...], preferred_element_type=jnp.float32)
        c += jnp.dot(b_ref[...], w_refs[2 * i + 1][...], preferred_element_type=jnp.float32)
        c = c.astype(jnp.bfloat16)
        for k, out_ref in enumerate(out_refs):

            @pl.when((at >= k * per) & (at < (k + 1) * per))
            def _():
                out_ref[at - k * per] = c


def finish_kernel(codes, heads, *rest):
    out_ref = rest[-1]
    me = place()
    core = lax.axis_index("head") & 1
    for r, slots in enumerate(codes):
        shares = rest[heads * r : heads * (r + 1)]
        for i, values in enumerate(slots):
            part = lookup(values, me)

            @pl.when(part != NONE)
            def _():
                width = shares[0].shape[2]
                for side in range(2):
                    c = shares[side][i].astype(jnp.float32)
                    for k in range(2 + side, heads, 2):
                        c += shares[k][i].astype(jnp.float32)
                    start = pl.multiple_of((2 * part + (core ^ side)) * width, LANES)
                    out_ref[:, pl.ds(start, width)] = c.astype(out_ref.dtype)


def reduce_plan(n, heads, sources, rounds):
    per = n // heads
    devices = [(s, h) for s in range(n) for h in range(heads)]
    plan = []
    for places in rounds:
        codes, pairs = [[] for _ in places], [[] for _ in range(heads)]
        owned = {d: [] for d in devices}
        for s, h in devices:
            counts = [0] * heads
            for i, p in enumerate(places):
                block = sources[s][p]
                k = (block // per) ^ h
                codes[i].append(k * per + counts[k])
                counts[k] += 1
                if not k:
                    owned[s, h].append(block % per)
            for k in range(heads):
                if counts[k]:
                    pairs[k].append((s * heads + h, s * heads + (h ^ k)))
        count = max(len(v) for v in owned.values())
        ends = [[v[i] if i < len(v) else NONE for v in owned.values()] for i in range(count)]
        plan.append((codes, pairs, count, ends))
    return plan


def ring_device(n, heads, queries, keys, values, doc_ids, span_order, out_weight):
    tok_rows = queries.shape[0]
    span = tok_rows // 2
    group = queries.shape[1] // DH
    width = out_weight.shape[1]
    per = n // heads
    hops = n // 2
    ring = ring_order(n)
    where = {s: i for i, s in enumerate(ring)}
    sources = []
    for s in range(n):
        row = [s]
        for hop in range(1, hops):
            row += [ring[(where[s] - hop) % n], ring[(where[s] + hop) % n]]
        sources.append(row + [ring[(where[s] + hops) % n]])

    def gather(pieces):
        def move(way, x):
            step = 1 if way == "up" else -1
            pairs = [(ring[p], ring[(p + step) % n]) for p in range(n)]
            return lax.ppermute(x, "seq", pairs)

        ups, downs = list(pieces), list(pieces)
        late = (len(pieces) + 1) // 2
        got = [list(pieces)]
        for hop in range(1, hops + 1):
            last = hop == hops
            for i in range(len(pieces)):
                if not last or i < late:
                    ups[i] = move("up", ups[i])
                if not last or i >= late:
                    downs[i] = move("dn", downs[i])
            if last:
                got.append(ups[:late] + downs[late:])
            else:
                got += [list(ups), list(downs)]
        return got

    both = jnp.concatenate([keys, values], axis=1)
    kv = [g[0] for g in gather([both])]
    out_weight, both = lax.optimization_barrier((out_weight, both))
    half = width // 2
    first = (lax.axis_index("head") & 1) == 0
    mine = jnp.where(first, out_weight[:, :half], out_weight[:, half:])
    other = jnp.where(first, out_weight[:, half:], out_weight[:, :half])
    beside = [(h, h ^ 1) for h in range(heads)]
    other = lax.ppermute(other, "head", beside)
    w = gather([mine, other])

    attended = pl.pallas_call(
        functools.partial(attention_kernel, n, span, group, sources),
        out_shape=jax.ShapeDtypeStruct((tok_rows, group * DH), jnp.bfloat16),
        in_specs=[SMEM, SMEM] + [VMEM] * (2 + n),
        out_specs=VMEM,
        scratch_shapes=[
            pltpu.VMEM((group * span, 2 * n * span), jnp.float32),
            pltpu.VMEM((group * span, span), jnp.float32),
            pltpu.VMEM((group * span, span), jnp.float32),
            pltpu.VMEM((group * span, DH), jnp.float32),
        ],
        compiler_params=limit(16),
        cost_estimate=pl.CostEstimate(
            flops=4 * group * tok_rows * n * tok_rows * DH,
            bytes_accessed=n * tok_rows * 4 * DH,
            transcendentals=group * tok_rows * n * tok_rows,
        ),
        name="attention",
    )(span_order, doc_ids, doc_ids.reshape(-1, span), queries, *kv)
    paired = lax.ppermute(attended, "head", beside)

    rounds = [list(range(n - 3)), [n - 3, n - 2], [n - 1]]
    shares, ends = [], []
    for r, (codes, pairs, count, end) in enumerate(reduce_plan(n, heads, sources, rounds)):
        pieces = [piece for p in rounds[r] for piece in w[p]]
        block = jax.ShapeDtypeStruct((count, tok_rows, half), jnp.bfloat16)
        made = pl.pallas_call(
            functools.partial(project_kernel, codes, per),
            out_shape=(block,) * heads,
            in_specs=[VMEM] * (2 + len(pieces)),
            out_specs=(VMEM,) * heads,
            compiler_params=limit(8),
            cost_estimate=pl.CostEstimate(
                flops=2 * tok_rows * group * DH * half * len(pieces),
                bytes_accessed=2 * group * DH * half * len(pieces),
                transcendentals=0,
            ),
            name="project",
        )(attended, paired, *pieces)
        shares.append(made[0])
        for k in range(1, heads):
            shares.append(lax.ppermute(made[k], ("seq", "head"), pairs[k]))
        ends.append(end)

    return pl.pallas_call(
        functools.partial(finish_kernel, ends, heads),
        out_shape=jax.ShapeDtypeStruct((tok_rows, per * width), jnp.bfloat16),
        in_specs=[VMEM] * len(shares),
        out_specs=VMEM,
        compiler_params=limit(8),
        name="finish",
    )(*shares)


def on_device(queries, keys, values, doc_ids, span_order, out_weight):
    tok_rows = queries.shape[0]
    span = tok_rows // 2
    local_heads = queries.shape[1] // DH
    local_kv = keys.shape[1] // DH
    group_size = local_heads // local_kv
    n_blocks = span_order.shape[0]
    scale = 1.0 / math.sqrt(DH)
    mine = lax.axis_index("seq")
    own_blocks = lax.dynamic_slice_in_dim(span_order, 2 * mine, 2, 0)
    local_rows = jnp.arange(tok_rows, dtype=jnp.int32)
    qpos = jnp.where(local_rows < span, own_blocks[0], own_blocks[1]) * span + local_rows % span
    qdoc = jnp.take(doc_ids, qpos)
    q_heads = queries.reshape(tok_rows, local_kv, group_size, DH)

    def update(state, kblk, vblk, kpos, kdoc):
        largest, total, summed = state
        count = kblk.shape[0]
        k_heads = kblk.reshape(count, local_kv, DH)
        v_heads = vblk.reshape(count, local_kv, DH)
        scores = (
            jnp.einsum("qhgd,khd->hgqk", q_heads, k_heads, preferred_element_type=jnp.float32)
            * scale
        )
        visible = (qdoc[:, None] == kdoc[None, :]) & (kpos[None, :] <= qpos[:, None])
        masked = jnp.where(visible, scores, jnp.float32(-1e30))
        new_largest = jnp.maximum(largest, jnp.max(masked, axis=-1))
        factor = jnp.exp(largest - new_largest)
        weights = jnp.where(visible, jnp.exp(masked - new_largest[..., None]), jnp.float32(0.0))
        total = total * factor + jnp.sum(weights, axis=-1)
        weights_b = weights.astype(jnp.bfloat16)
        added = jnp.einsum("hgqk,khd->qhgd", weights_b, v_heads, preferred_element_type=jnp.float32)
        summed = summed * jnp.transpose(factor, (2, 0, 1))[..., None] + added
        return (new_largest, total, summed)

    initial = (
        jnp.full((local_kv, group_size, tok_rows), -1e30, jnp.float32),
        jnp.zeros((local_kv, group_size, tok_rows), jnp.float32),
        jnp.zeros((tok_rows, local_kv, group_size, DH), jnp.float32),
    )
    state = initial
    kpiece = lax.all_gather(keys, "seq", axis=0, tiled=True)
    vpiece = lax.all_gather(values, "seq", axis=0, tiled=True)
    count = kpiece.shape[0]
    width = math.gcd(count, 1024)
    steps = count // width
    rows = jnp.arange(count, dtype=jnp.int32)
    match = (rows // span)[:, None] == jnp.arange(n_blocks, dtype=jnp.int32)[None, :]
    owner = jnp.sum(jnp.where(match, span_order[None, :], 0), axis=1)
    kpos = owner * span + rows % span
    kdoc = jnp.take(doc_ids, kpos)
    kparts = kpiece.reshape(steps, width, kpiece.shape[1])
    vparts = vpiece.reshape(steps, width, vpiece.shape[1])

    def one_step(carry, items):
        kblk, vblk, pblk, dblk = items
        carry = update(carry, kblk, vblk, pblk, dblk)
        return (carry, None)

    state, _ = lax.scan(
        one_step, state, (kparts, vparts, kpos.reshape(steps, width), kdoc.reshape(steps, width))
    )
    _, total, summed = state
    attended = (summed / jnp.transpose(total, (2, 0, 1))[..., None]).astype(jnp.bfloat16)
    attended = attended.reshape(tok_rows, local_heads * DH)
    partial_out = jnp.dot(
        attended,
        lax.all_gather(out_weight, "seq", axis=1, tiled=True),
        preferred_element_type=jnp.float32,
    )
    return lax.psum_scatter(
        partial_out.astype(jnp.bfloat16), "head", scatter_dimension=1, tiled=True
    )


def solution(mesh):
    n, heads = mesh.shape["seq"], mesh.shape["head"]

    def on_each(queries, keys, values, doc_ids, span_order, out_weight):
        span = queries.shape[0] // 2
        ring = (
            4 <= n <= 16
            and n % 2 == 0
            and n % heads == 0
            and heads & (heads - 1) == 0
            and keys.shape[1] == DH
            and span % LANES == 0
            and out_weight.shape[1] % (2 * LANES) == 0
        )
        args = (queries, keys, values, doc_ids, span_order, out_weight)
        if not ring:
            return on_device(*args)
        return ring_device(n, heads, *args)

    return jax.shard_map(
        on_each,
        mesh=mesh,
        in_specs=(P("seq", "head"), P("seq", "head"), P("seq", "head"), P(), P(), P("head", "seq")),
        out_specs=P("seq", "head"),
        check_vma=False,
    )
```

```python
import functools
import math

import jax
import jax.numpy as jnp
from jax import lax
from jax.experimental import pallas as pl
from jax.experimental.pallas import tpu as pltpu
from jax.sharding import PartitionSpec as P


DH = 128
LANES = 128
NONE = -1000
VMEM = pl.BlockSpec(memory_space=pltpu.VMEM)
SMEM = pl.BlockSpec(memory_space=pltpu.SMEM)
NONE, KEEP = 15, 8


def limit(mib):
    return pltpu.CompilerParams(vmem_limit_bytes=mib * 2**20)


def lookup(values, index):
    words = []
    for i in range(0, len(values), 8):
        word = sum(v << 4 * k for k, v in enumerate(values[i : i + 8]))
        words.append(word - 2**32 if word >= 2**31 else word)
    word = jnp.int32(words[0])
    for i in range(1, len(words)):
        word = jnp.where(index // 8 == i, jnp.int32(words[i]), word)
    return (word >> (4 * (index % 8))) & 15


def ring_order(n):
    return list(range(0, n, 2)) + list(range(n - 1, 0, -2))


def attention_kernel(span, group, sources, first, order_ref, docid_ref, docs_ref, q_ref, *rest):
    many = len(sources[0])
    kv_refs, rest = rest[:many], rest[many:]
    if first:
        top_ref, sum_ref, mix_ref, s_ref, m_ref = rest
    else:
        top_in, sum_in, mix_in, out_ref, s_ref, m_ref, sum_ref, mix_ref = rest
    base2 = math.log2(math.e) / math.sqrt(DH)
    mine = lax.axis_index("seq")
    dims = (((1,), (1,)), ((), ()))
    kposs = []
    for i in range(many):
        source = lookup([row[i] for row in sources], mine)
        kposs += [order_ref[2 * source], order_ref[2 * source + 1]]

    for part in range(2):
        rows = pl.ds(part * span, span)
        qpos = order_ref[2 * mine + part]
        q = jnp.concatenate(
            [q_ref[rows, h * DH : (h + 1) * DH] for h in range(group)], axis=0
        )
        qdoc = jnp.transpose(
            jnp.broadcast_to(docs_ref[pl.ds(qpos, 1), :], (span, span)).astype(jnp.float32)
        )
        qfirst = docid_ref[qpos * span]
        ahead = lax.broadcasted_iota(jnp.int32, (span, span), 1) - lax.broadcasted_iota(
            jnp.int32, (span, span), 0
        )
        m_ref[...] = jnp.full_like(m_ref, -1e30)
        lives = [(k <= qpos) & (docid_ref[k * span + span - 1] >= qfirst) for k in kposs]

        for j in range(2 * many):

            @pl.when(lives[j])
            def _():
                k = kv_refs[j // 2][(j % 2) * span : (j % 2 + 1) * span, :DH]
                s = lax.dot_general(q, k, dims, preferred_element_type=jnp.float32)
                kdoc = docs_ref[pl.ds(kposs[j], 1), :].astype(jnp.float32)
                visible = (qdoc == kdoc) & (ahead <= (qpos - kposs[j]) * span)
                s = jnp.where(visible[None], s.reshape(group, span, span), -1e30)
                s = s.reshape(group * span, span)
                s_ref[:, j * span : (j + 1) * span] = s
                m_ref[...] = jnp.maximum(m_ref[...], s)

        largest = jnp.max(m_ref[...], axis=1, keepdims=True) * base2
        if first:
            top_ref[part] = jnp.broadcast_to(largest, m_ref.shape)
            sum_ref[part] = jnp.zeros_like(m_ref)
            mix_ref[part] = jnp.zeros_like(m_ref)
        else:
            before = top_in[part]
            largest = jnp.maximum(before, largest)
            fade = jnp.exp2(before - largest)
            sum_ref[part] = sum_in[part] * fade
            mix_ref[part] = mix_in[part] * fade

        for j in range(2 * many):

            @pl.when(lives[j])
            def _():
                p = jnp.exp2(s_ref[:, j * span : (j + 1) * span] * base2 - largest)
                sum_ref[part] += p
                v = kv_refs[j // 2][(j % 2) * span : (j % 2 + 1) * span, DH:]
                mix_ref[part] += jnp.dot(
                    p.astype(jnp.bfloat16), v, preferred_element_type=jnp.float32
                )

        if not first:
            total = jnp.sum(sum_ref[part], axis=1, keepdims=True)
            attended = (mix_ref[part] / total).astype(jnp.bfloat16)
            for h in range(group):
                out_ref[rows, h * DH : (h + 1) * DH] = attended[h * span : (h + 1) * span]


def place():
    return lax.axis_index("seq") * lax.axis_size("head") + lax.axis_index("head")


def project_kernel(codes, a_ref, b_ref, *rest):
    w_refs, (send_ref, keep_ref) = rest[:-2], rest[-2:]
    me = place()
    for i, values in enumerate(codes):
        at = lookup(values, me)
        c = jnp.dot(a_ref[...], w_refs[2 * i][...], preferred_element_type=jnp.float32)
        c += jnp.dot(b_ref[...], w_refs[2 * i + 1][...], preferred_element_type=jnp.float32)
        c = c.astype(jnp.bfloat16)

        @pl.when(at < KEEP)
        def _():
            send_ref[at] = c

        @pl.when(at >= KEEP)
        def _():
            keep_ref[at - KEEP] = c


def fold_kernel(codes, per, *rest):
    kept, came, (own_ref, send_ref) = rest[: len(codes)], rest[len(codes) : -2], rest[-2:]
    me = place()
    for r, slots in enumerate(codes):
        for i, values in enumerate(slots):
            at = lookup(values, me)

            @pl.when(at != NONE)
            def _():
                c = kept[r][i].astype(jnp.float32) + came[r][i].astype(jnp.float32)
                c = c.astype(jnp.bfloat16)

                @pl.when(at < per)
                def _():
                    own_ref[at] = c

                @pl.when(at >= per)
                def _():
                    send_ref[at - per] = c


def finish_kernel(own_ref, came_ref, out_ref):
    core = lax.axis_index("head") & 1
    per, _, half = own_ref.shape
    for part in range(per):
        for ref, side in ((own_ref, core), (came_ref, 1 - core)):
            start = pl.multiple_of((2 * part + side) * half, LANES)
            out_ref[:, pl.ds(start, half)] = ref[part]


def reduce_plan(n, heads, sources, rounds):
    per = n // heads
    devices = [(s, h) for s in range(n) for h in range(heads)]
    plan = []
    for places in rounds:
        codes, pairs = [[] for _ in places], []
        kept = {d: [] for d in devices}
        for s, h in devices:
            sent = 0
            for i, p in enumerate(places):
                block = sources[s][p]
                away = (block // per) ^ h
                if away & 2:
                    codes[i].append(sent)
                    sent += 1
                else:
                    codes[i].append(KEEP + len(kept[s, h]))
                    kept[s, h].append(block % per + per * (away & 1))
            if sent:
                pairs.append((s * heads + h, s * heads + (h ^ 2)))
        count = max(len(v) for v in kept.values())
        ends = [[v[i] if i < len(v) else NONE for v in kept.values()] for i in range(count)]
        plan.append((codes, pairs, count, ends))
    return plan


def ring_device(n, heads, queries, keys, values, doc_ids, span_order, out_weight):
    tok_rows = queries.shape[0]
    span = tok_rows // 2
    group = queries.shape[1] // DH
    width = out_weight.shape[1]
    per = n // heads
    hops = n // 2
    ring = ring_order(n)
    where = {s: i for i, s in enumerate(ring)}
    sources = []
    for s in range(n):
        row = [s]
        for hop in range(1, hops):
            row += [ring[(where[s] - hop) % n], ring[(where[s] + hop) % n]]
        sources.append(row + [ring[(where[s] + hops) % n]])

    def gather(pieces):
        def move(way, x):
            step = 1 if way == "up" else -1
            pairs = [(ring[p], ring[(p + step) % n]) for p in range(n)]
            return lax.ppermute(x, "seq", pairs)

        ups, downs = list(pieces), list(pieces)
        late = (len(pieces) + 1) // 2
        got = [list(pieces)]
        for hop in range(1, hops + 1):
            last = hop == hops
            for i in range(len(pieces)):
                if not last or i < late:
                    ups[i] = move("up", ups[i])
                if not last or i >= late:
                    downs[i] = move("dn", downs[i])
            if last:
                got.append(ups[:late] + downs[late:])
            else:
                got += [list(ups), list(downs)]
        return got

    both = jnp.concatenate([keys, values], axis=1)
    kv = [g[0] for g in gather([both])]
    out_weight, both = lax.optimization_barrier((out_weight, both))
    half = width // 2
    first = (lax.axis_index("head") & 1) == 0
    mine = jnp.where(first, out_weight[:, :half], out_weight[:, half:])
    other = jnp.where(first, out_weight[:, half:], out_weight[:, :half])
    beside = [(h, h ^ 1) for h in range(heads)]
    other = lax.ppermute(other, "head", beside)
    w = gather([mine, other])

    def attend(stage, slots, state, out_shape):
        first = stage == 0
        block = pltpu.VMEM((group * span, span), jnp.float32)
        states = pltpu.VMEM((2, group * span, span), jnp.float32)
        share = 2 * len(slots) * group * tok_rows * tok_rows
        args = [queries] + [kv[i] for i in slots] + state
        return pl.pallas_call(
            functools.partial(
                attention_kernel, span, group, [[row[i] for i in slots] for row in sources], first
            ),
            out_shape=out_shape,
            in_specs=[SMEM, SMEM] + [VMEM] * (1 + len(args)),
            out_specs=jax.tree.map(lambda _: VMEM, out_shape),
            scratch_shapes=[pltpu.VMEM((group * span, 2 * len(slots) * span), jnp.float32), block]
            + ([] if first else [states, states]),
            compiler_params=limit(16),
            cost_estimate=pl.CostEstimate(
                flops=2 * share * DH,
                bytes_accessed=len(slots) * tok_rows * 4 * DH,
                transcendentals=share,
            ),
            name="attend",
        )(span_order, doc_ids, doc_ids.reshape(-1, span), *args)

    memory = jax.ShapeDtypeStruct((2, group * span, span), jnp.float32)
    state = attend(0, range(n - 1), [], (memory,) * 3)
    attended = attend(
        1, [n - 1], list(state), jax.ShapeDtypeStruct((tok_rows, group * DH), jnp.bfloat16)
    )
    paired = lax.ppermute(attended, "head", beside)

    def block(count):
        return jax.ShapeDtypeStruct((count, tok_rows, half), jnp.bfloat16)

    rounds = [list(range(n - 3)), [n - 3, n - 2], [n - 1]]
    kept, came, ends = [], [], []
    for r, (codes, pairs, count, end) in enumerate(reduce_plan(n, heads, sources, rounds)):
        pieces = [piece for p in rounds[r] for piece in w[p]]
        send, keep = pl.pallas_call(
            functools.partial(project_kernel, codes),
            out_shape=(block(count), block(count)),
            in_specs=[VMEM] * (2 + len(pieces)),
            out_specs=(VMEM, VMEM),
            compiler_params=limit(8),
            cost_estimate=pl.CostEstimate(
                flops=2 * tok_rows * group * DH * half * len(pieces),
                bytes_accessed=2 * group * DH * half * len(pieces),
                transcendentals=0,
            ),
            name="project",
        )(attended, paired, *pieces)
        came.append(lax.ppermute(send, ("seq", "head"), pairs))
        kept.append(keep)
        ends.append(end)

    own, send = pl.pallas_call(
        functools.partial(fold_kernel, ends, per),
        out_shape=(block(per), block(per)),
        in_specs=[VMEM] * (2 * len(ends)),
        out_specs=(VMEM, VMEM),
        compiler_params=limit(8),
        name="fold",
    )(*kept, *came)
    joined = lax.ppermute(send, "head", beside)
    return pl.pallas_call(
        finish_kernel,
        out_shape=jax.ShapeDtypeStruct((tok_rows, per * width), jnp.bfloat16),
        in_specs=[VMEM, VMEM],
        out_specs=VMEM,
        compiler_params=limit(8),
        name="finish",
    )(own, joined)


def on_device(queries, keys, values, doc_ids, span_order, out_weight):
    tok_rows = queries.shape[0]
    span = tok_rows // 2
    local_heads = queries.shape[1] // DH
    local_kv = keys.shape[1] // DH
    group_size = local_heads // local_kv
    n_blocks = span_order.shape[0]
    scale = 1.0 / math.sqrt(DH)
    mine = lax.axis_index("seq")
    own_blocks = lax.dynamic_slice_in_dim(span_order, 2 * mine, 2, 0)
    local_rows = jnp.arange(tok_rows, dtype=jnp.int32)
    qpos = jnp.where(local_rows < span, own_blocks[0], own_blocks[1]) * span + local_rows % span
    qdoc = jnp.take(doc_ids, qpos)
    q_heads = queries.reshape(tok_rows, local_kv, group_size, DH)

    def update(state, kblk, vblk, kpos, kdoc):
        largest, total, summed = state
        count = kblk.shape[0]
        k_heads = kblk.reshape(count, local_kv, DH)
        v_heads = vblk.reshape(count, local_kv, DH)
        scores = (
            jnp.einsum("qhgd,khd->hgqk", q_heads, k_heads, preferred_element_type=jnp.float32)
            * scale
        )
        visible = (qdoc[:, None] == kdoc[None, :]) & (kpos[None, :] <= qpos[:, None])
        masked = jnp.where(visible, scores, jnp.float32(-1e30))
        new_largest = jnp.maximum(largest, jnp.max(masked, axis=-1))
        factor = jnp.exp(largest - new_largest)
        weights = jnp.where(visible, jnp.exp(masked - new_largest[..., None]), jnp.float32(0.0))
        total = total * factor + jnp.sum(weights, axis=-1)
        weights_b = weights.astype(jnp.bfloat16)
        added = jnp.einsum("hgqk,khd->qhgd", weights_b, v_heads, preferred_element_type=jnp.float32)
        summed = summed * jnp.transpose(factor, (2, 0, 1))[..., None] + added
        return (new_largest, total, summed)

    initial = (
        jnp.full((local_kv, group_size, tok_rows), -1e30, jnp.float32),
        jnp.zeros((local_kv, group_size, tok_rows), jnp.float32),
        jnp.zeros((tok_rows, local_kv, group_size, DH), jnp.float32),
    )
    state = initial
    kpiece = lax.all_gather(keys, "seq", axis=0, tiled=True)
    vpiece = lax.all_gather(values, "seq", axis=0, tiled=True)
    count = kpiece.shape[0]
    width = math.gcd(count, 1024)
    steps = count // width
    rows = jnp.arange(count, dtype=jnp.int32)
    match = (rows // span)[:, None] == jnp.arange(n_blocks, dtype=jnp.int32)[None, :]
    owner = jnp.sum(jnp.where(match, span_order[None, :], 0), axis=1)
    kpos = owner * span + rows % span
    kdoc = jnp.take(doc_ids, kpos)
    kparts = kpiece.reshape(steps, width, kpiece.shape[1])
    vparts = vpiece.reshape(steps, width, vpiece.shape[1])

    def one_step(carry, items):
        kblk, vblk, pblk, dblk = items
        carry = update(carry, kblk, vblk, pblk, dblk)
        return (carry, None)

    state, _ = lax.scan(
        one_step, state, (kparts, vparts, kpos.reshape(steps, width), kdoc.reshape(steps, width))
    )
    _, total, summed = state
    attended = (summed / jnp.transpose(total, (2, 0, 1))[..., None]).astype(jnp.bfloat16)
    attended = attended.reshape(tok_rows, local_heads * DH)
    partial_out = jnp.dot(
        attended,
        lax.all_gather(out_weight, "seq", axis=1, tiled=True),
        preferred_element_type=jnp.float32,
    )
    return lax.psum_scatter(
        partial_out.astype(jnp.bfloat16), "head", scatter_dimension=1, tiled=True
    )


def solution(mesh):
    n, heads = mesh.shape["seq"], mesh.shape["head"]

    def on_each(queries, keys, values, doc_ids, span_order, out_weight):
        span = queries.shape[0] // 2
        ring = (
            4 <= n <= 16
            and n % 2 == 0
            and n % heads == 0
            and heads == 4
            and keys.shape[1] == DH
            and span % LANES == 0
            and out_weight.shape[1] % (2 * LANES) == 0
        )
        args = (queries, keys, values, doc_ids, span_order, out_weight)
        if not ring:
            return on_device(*args)
        return ring_device(n, heads, *args)

    return jax.shard_map(
        on_each,
        mesh=mesh,
        in_specs=(P("seq", "head"), P("seq", "head"), P("seq", "head"), P(), P(), P("head", "seq")),
        out_specs=P("seq", "head"),
        check_vma=False,
    )
```

```python
import functools
import math

import jax
import jax.numpy as jnp
from jax import lax
from jax.experimental import pallas as pl
from jax.experimental.pallas import tpu as pltpu
from jax.sharding import PartitionSpec as P


DH = 128
LANES = 128
NONE = -1000
VMEM = pl.BlockSpec(memory_space=pltpu.VMEM)
SMEM = pl.BlockSpec(memory_space=pltpu.SMEM)
SEND, KEEP, HOLD, NONE = 0, 5, 10, 15


def limit(mib):
    return pltpu.CompilerParams(vmem_limit_bytes=mib * 2**20)


def lookup(values, index):
    words = []
    for i in range(0, len(values), 8):
        word = sum(v << 4 * k for k, v in enumerate(values[i : i + 8]))
        words.append(word - 2**32 if word >= 2**31 else word)
    word = jnp.int32(words[0])
    for i in range(1, len(words)):
        word = jnp.where(index // 8 == i, jnp.int32(words[i]), word)
    return (word >> (4 * (index % 8))) & 15


def ring_order(n):
    return list(range(0, n, 2)) + list(range(n - 1, 0, -2))


def attention_kernel(span, group, sources, first, order_ref, docid_ref, docs_ref, q_ref, *rest):
    many = len(sources[0])
    split = 1 if first else 2
    kv_refs, rest = rest[: many * split], rest[many * split :]
    spans = [(ref, at) for ref in kv_refs for at in range(0, ref.shape[0], span)]
    if first:
        top_ref, sum_ref, mix_ref, s_ref, m_ref = rest
    else:
        top_in, sum_in, mix_in, out_ref, s_ref, m_ref, sum_ref, mix_ref = rest
    base2 = math.log2(math.e) / math.sqrt(DH)
    mine = lax.axis_index("seq")
    dims = (((1,), (1,)), ((), ()))
    kposs = []
    for i in range(many):
        source = lookup([row[i] for row in sources], mine)
        kposs += [order_ref[2 * source], order_ref[2 * source + 1]]

    for part in range(2):
        rows = pl.ds(part * span, span)
        qpos = order_ref[2 * mine + part]
        q = jnp.concatenate(
            [q_ref[rows, h * DH : (h + 1) * DH] for h in range(group)], axis=0
        )
        qdoc = jnp.transpose(
            jnp.broadcast_to(docs_ref[pl.ds(qpos, 1), :], (span, span)).astype(jnp.float32)
        )
        qfirst = docid_ref[qpos * span]
        ahead = lax.broadcasted_iota(jnp.int32, (span, span), 1) - lax.broadcasted_iota(
            jnp.int32, (span, span), 0
        )
        m_ref[...] = jnp.full_like(m_ref, -1e30)
        lives = [(k <= qpos) & (docid_ref[k * span + span - 1] >= qfirst) for k in kposs]

        for j in range(2 * many):

            @pl.when(lives[j])
            def _():
                k = spans[j][0][spans[j][1] : spans[j][1] + span, :DH]
                s = lax.dot_general(q, k, dims, preferred_element_type=jnp.float32)
                kdoc = docs_ref[pl.ds(kposs[j], 1), :].astype(jnp.float32)
                visible = (qdoc == kdoc) & (ahead <= (qpos - kposs[j]) * span)
                s = jnp.where(visible[None], s.reshape(group, span, span), -1e30)
                s = s.reshape(group * span, span)
                s_ref[:, j * span : (j + 1) * span] = s
                m_ref[...] = jnp.maximum(m_ref[...], s)

        largest = jnp.max(m_ref[...], axis=1, keepdims=True) * base2
        if first:
            top_ref[part] = jnp.broadcast_to(largest, m_ref.shape)
            sum_ref[part] = jnp.zeros_like(m_ref)
            mix_ref[part] = jnp.zeros_like(m_ref)
        else:
            before = top_in[part]
            largest = jnp.maximum(before, largest)
            fade = jnp.exp2(before - largest)
            sum_ref[part] = sum_in[part] * fade
            mix_ref[part] = mix_in[part] * fade

        for j in range(2 * many):

            @pl.when(lives[j])
            def _():
                p = jnp.exp2(s_ref[:, j * span : (j + 1) * span] * base2 - largest)
                sum_ref[part] += p
                v = spans[j][0][spans[j][1] : spans[j][1] + span, DH:]
                mix_ref[part] += jnp.dot(
                    p.astype(jnp.bfloat16), v, preferred_element_type=jnp.float32
                )

        if not first:
            total = jnp.sum(sum_ref[part], axis=1, keepdims=True)
            attended = (mix_ref[part] / total).astype(jnp.bfloat16)
            for h in range(group):
                out_ref[rows, h * DH : (h + 1) * DH] = attended[h * span : (h + 1) * span]


def place():
    return lax.axis_index("seq") * lax.axis_size("head") + lax.axis_index("head")


def project_kernel(codes, moved, a_ref, b_ref, *rest):
    w_refs, rest = rest[: 2 * len(codes)], rest[2 * len(codes) :]
    if moved:
        held_ref, rest = rest[0], rest[1:]
    me = place()

    def put(at, c):
        for low, ref in zip((SEND, KEEP, HOLD), rest):

            @pl.when((at >= low) & (at < low + ref.shape[0]))
            def _():
                ref[at - low] = c

    for i, values in enumerate(moved):
        put(lookup(values, me), held_ref[i])
    for i, values in enumerate(codes):
        c = jnp.dot(a_ref[...], w_refs[2 * i][...], preferred_element_type=jnp.float32)
        c += jnp.dot(b_ref[...], w_refs[2 * i + 1][...], preferred_element_type=jnp.float32)
        put(lookup(values, me), c.astype(jnp.bfloat16))


def fold_kernel(codes, per, *rest):
    kept, came, (own_ref, send_ref) = rest[: len(codes)], rest[len(codes) : -2], rest[-2:]
    me = place()
    for r, slots in enumerate(codes):
        for i, values in enumerate(slots):
            at = lookup(values, me)

            @pl.when(at != NONE)
            def _():
                c = kept[r][i].astype(jnp.float32) + came[r][i].astype(jnp.float32)
                c = c.astype(jnp.bfloat16)

                @pl.when(at < per)
                def _():
                    own_ref[at] = c

                @pl.when(at >= per)
                def _():
                    send_ref[at - per] = c


def finish_kernel(own_ref, came_ref, out_ref):
    core = lax.axis_index("head") & 1
    per, _, half = own_ref.shape
    for part in range(per):
        for ref, side in ((own_ref, core), (came_ref, 1 - core)):
            start = pl.multiple_of((2 * part + side) * half, LANES)
            out_ref[:, pl.ds(start, half)] = ref[part]


def reduce_plan(n, heads, sources, rounds):
    per = n // heads
    devices = [(s, h) for s in range(n) for h in range(heads)]
    first = n // 2 - sum(len(places) for places in rounds[1:])
    caps = [max(1, first)] + [len(places) for places in rounds[1:]]
    turns = {}
    for s in range(n):
        for owners in (0, 2):
            room = list(caps)
            for r, places in enumerate(rounds):
                for p in places:
                    if (sources[s][p] // per) & 2 == owners:
                        at = next(k for k in range(r, len(caps)) if room[k])
                        room[at] -= 1
                        turns[s, p] = at
    plan = []
    held = {d: [] for d in devices}
    for r, places in enumerate(rounds):
        codes, moved = [[] for _ in places], [[] for _ in range(max(map(len, held.values())))]
        kept, later = {d: [] for d in devices}, {d: [] for d in devices}
        for s, h in devices:
            sent = 0
            jobs = [(moved[i], p) for i, p in enumerate(held[s, h])]
            jobs += [(codes[i], p) for i, p in enumerate(places)]
            for row, p in jobs:
                block = sources[s][p]
                away = (block // per) ^ h
                if turns[s, p] > r:
                    row.append(HOLD + len(later[s, h]))
                    later[s, h].append(p)
                elif away & 2:
                    row.append(SEND + sent)
                    sent += 1
                else:
                    row.append(KEEP + len(kept[s, h]))
                    kept[s, h].append(block % per + per * (away & 1))
            for row in moved[len(held[s, h]) :]:
                row.append(NONE)
        held = later
        ends = [[v[i] if i < len(v) else NONE for v in kept.values()] for i in range(caps[r])]
        plan.append((codes, moved, caps[r], max(map(len, held.values())), ends))
    return plan


def ring_device(n, heads, queries, keys, values, doc_ids, span_order, out_weight):
    tok_rows = queries.shape[0]
    span = tok_rows // 2
    group = queries.shape[1] // DH
    width = out_weight.shape[1]
    per = n // heads
    hops = n // 2
    ring = ring_order(n)
    where = {s: i for i, s in enumerate(ring)}
    sources = []
    for s in range(n):
        row = [s]
        for hop in range(1, hops):
            row += [ring[(where[s] - hop) % n], ring[(where[s] + hop) % n]]
        sources.append(row + [ring[(where[s] + hops) % n]])

    def gather(pieces):
        def move(way, x):
            step = 1 if way == "up" else -1
            pairs = [(ring[p], ring[(p + step) % n]) for p in range(n)]
            return lax.ppermute(x, "seq", pairs)

        ups, downs = list(pieces), list(pieces)
        got = [list(pieces)]
        for _ in range(1, hops):
            for i in range(len(pieces)):
                ups[i] = move("up", ups[i])
                downs[i] = move("dn", downs[i])
            got += [list(ups), list(downs)]
        if len(pieces) == 1:
            rows = pieces[0].shape[0] // 2
            ups, downs = [ups[0][:rows], None], [None, downs[0][rows:]]
        got.append([move("up", ups[0]), move("dn", downs[1])])
        return got

    kv = gather([jnp.concatenate([keys, values], axis=1)])
    half = width // 2
    first = (lax.axis_index("head") & 1) == 0
    mine = jnp.where(first, out_weight[:, :half], out_weight[:, half:])
    other = jnp.where(first, out_weight[:, half:], out_weight[:, :half])
    beside = [(h, h ^ 1) for h in range(heads)]
    other = lax.ppermute(other, "head", beside)
    w = gather([mine, other])

    def attend(stage, slots, state, out_shape):
        first = stage == 0
        block = pltpu.VMEM((group * span, span), jnp.float32)
        states = pltpu.VMEM((2, group * span, span), jnp.float32)
        share = 2 * len(slots) * group * tok_rows * tok_rows
        args = [queries] + [piece for i in slots for piece in kv[i]] + state
        return pl.pallas_call(
            functools.partial(
                attention_kernel, span, group, [[row[i] for i in slots] for row in sources], first
            ),
            out_shape=out_shape,
            in_specs=[SMEM, SMEM] + [VMEM] * (1 + len(args)),
            out_specs=jax.tree.map(lambda _: VMEM, out_shape),
            scratch_shapes=[pltpu.VMEM((group * span, 2 * len(slots) * span), jnp.float32), block]
            + ([] if first else [states, states]),
            compiler_params=limit(16),
            cost_estimate=pl.CostEstimate(
                flops=2 * share * DH,
                bytes_accessed=len(slots) * tok_rows * 4 * DH,
                transcendentals=share,
            ),
            name="attend",
        )(span_order, doc_ids, doc_ids.reshape(-1, span), *args)

    memory = jax.ShapeDtypeStruct((2, group * span, span), jnp.float32)
    state = attend(0, range(n - 1), [], (memory,) * 3)
    attended = attend(
        1, [n - 1], list(state), jax.ShapeDtypeStruct((tok_rows, group * DH), jnp.bfloat16)
    )
    paired = lax.ppermute(attended, "head", beside)

    def block(count):
        return jax.ShapeDtypeStruct((count, tok_rows, half), jnp.bfloat16)

    rounds = [list(range(n - 3)), [n - 3, n - 2], [n - 1]]
    across = [(h, h ^ 2) for h in range(heads)]
    kept, came, ends, held = [], [], [], []
    for r, (codes, moved, count, hold, end) in enumerate(
        reduce_plan(n, heads, sources, rounds)
    ):
        pieces = [piece for p in rounds[r] for piece in w[p]]
        outs = (block(count), block(count)) + ((block(hold),) if hold else ())
        send, keep, *rest = pl.pallas_call(
            functools.partial(project_kernel, codes, moved),
            out_shape=outs,
            in_specs=[VMEM] * (2 + len(pieces) + len(held)),
            out_specs=(VMEM,) * len(outs),
            compiler_params=limit(8),
            cost_estimate=pl.CostEstimate(
                flops=2 * tok_rows * group * DH * half * len(pieces),
                bytes_accessed=2 * group * DH * half * len(pieces),
                transcendentals=0,
            ),
            name="project",
        )(attended, paired, *pieces, *held)
        came.append(lax.ppermute(send, "head", across))
        held = rest
        kept.append(keep)
        ends.append(end)

    own, send = pl.pallas_call(
        functools.partial(fold_kernel, ends, per),
        out_shape=(block(per), block(per)),
        in_specs=[VMEM] * (2 * len(ends)),
        out_specs=(VMEM, VMEM),
        compiler_params=limit(8),
        name="fold",
    )(*kept, *came)
    joined = lax.ppermute(send, "head", beside)
    return pl.pallas_call(
        finish_kernel,
        out_shape=jax.ShapeDtypeStruct((tok_rows, per * width), jnp.bfloat16),
        in_specs=[VMEM, VMEM],
        out_specs=VMEM,
        compiler_params=limit(8),
        name="finish",
    )(own, joined)


def on_device(queries, keys, values, doc_ids, span_order, out_weight):
    tok_rows = queries.shape[0]
    span = tok_rows // 2
    local_heads = queries.shape[1] // DH
    local_kv = keys.shape[1] // DH
    group_size = local_heads // local_kv
    n_blocks = span_order.shape[0]
    scale = 1.0 / math.sqrt(DH)
    mine = lax.axis_index("seq")
    own_blocks = lax.dynamic_slice_in_dim(span_order, 2 * mine, 2, 0)
    local_rows = jnp.arange(tok_rows, dtype=jnp.int32)
    qpos = jnp.where(local_rows < span, own_blocks[0], own_blocks[1]) * span + local_rows % span
    qdoc = jnp.take(doc_ids, qpos)
    q_heads = queries.reshape(tok_rows, local_kv, group_size, DH)

    def update(state, kblk, vblk, kpos, kdoc):
        largest, total, summed = state
        count = kblk.shape[0]
        k_heads = kblk.reshape(count, local_kv, DH)
        v_heads = vblk.reshape(count, local_kv, DH)
        scores = (
            jnp.einsum("qhgd,khd->hgqk", q_heads, k_heads, preferred_element_type=jnp.float32)
            * scale
        )
        visible = (qdoc[:, None] == kdoc[None, :]) & (kpos[None, :] <= qpos[:, None])
        masked = jnp.where(visible, scores, jnp.float32(-1e30))
        new_largest = jnp.maximum(largest, jnp.max(masked, axis=-1))
        factor = jnp.exp(largest - new_largest)
        weights = jnp.where(visible, jnp.exp(masked - new_largest[..., None]), jnp.float32(0.0))
        total = total * factor + jnp.sum(weights, axis=-1)
        weights_b = weights.astype(jnp.bfloat16)
        added = jnp.einsum("hgqk,khd->qhgd", weights_b, v_heads, preferred_element_type=jnp.float32)
        summed = summed * jnp.transpose(factor, (2, 0, 1))[..., None] + added
        return (new_largest, total, summed)

    initial = (
        jnp.full((local_kv, group_size, tok_rows), -1e30, jnp.float32),
        jnp.zeros((local_kv, group_size, tok_rows), jnp.float32),
        jnp.zeros((tok_rows, local_kv, group_size, DH), jnp.float32),
    )
    state = initial
    kpiece = lax.all_gather(keys, "seq", axis=0, tiled=True)
    vpiece = lax.all_gather(values, "seq", axis=0, tiled=True)
    count = kpiece.shape[0]
    width = math.gcd(count, 1024)
    steps = count // width
    rows = jnp.arange(count, dtype=jnp.int32)
    match = (rows // span)[:, None] == jnp.arange(n_blocks, dtype=jnp.int32)[None, :]
    owner = jnp.sum(jnp.where(match, span_order[None, :], 0), axis=1)
    kpos = owner * span + rows % span
    kdoc = jnp.take(doc_ids, kpos)
    kparts = kpiece.reshape(steps, width, kpiece.shape[1])
    vparts = vpiece.reshape(steps, width, vpiece.shape[1])

    def one_step(carry, items):
        kblk, vblk, pblk, dblk = items
        carry = update(carry, kblk, vblk, pblk, dblk)
        return (carry, None)

    state, _ = lax.scan(
        one_step, state, (kparts, vparts, kpos.reshape(steps, width), kdoc.reshape(steps, width))
    )
    _, total, summed = state
    attended = (summed / jnp.transpose(total, (2, 0, 1))[..., None]).astype(jnp.bfloat16)
    attended = attended.reshape(tok_rows, local_heads * DH)
    partial_out = jnp.dot(
        attended,
        lax.all_gather(out_weight, "seq", axis=1, tiled=True),
        preferred_element_type=jnp.float32,
    )
    return lax.psum_scatter(
        partial_out.astype(jnp.bfloat16), "head", scatter_dimension=1, tiled=True
    )


def solution(mesh):
    n, heads = mesh.shape["seq"], mesh.shape["head"]

    def on_each(queries, keys, values, doc_ids, span_order, out_weight):
        span = queries.shape[0] // 2
        ring = (
            4 <= n <= 16
            and n % 2 == 0
            and n % heads == 0
            and heads == 4
            and keys.shape[1] == DH
            and span % LANES == 0
            and out_weight.shape[1] % (2 * LANES) == 0
        )
        args = (queries, keys, values, doc_ids, span_order, out_weight)
        if not ring:
            return on_device(*args)
        return ring_device(n, heads, *args)

    return jax.shard_map(
        on_each,
        mesh=mesh,
        in_specs=(P("seq", "head"), P("seq", "head"), P("seq", "head"), P(), P(), P("head", "seq")),
        out_specs=P("seq", "head"),
        check_vma=False,
    )
```

```python
import functools
import math

import jax
import jax.numpy as jnp
from jax import lax
from jax.experimental import pallas as pl
from jax.experimental.pallas import tpu as pltpu
from jax.sharding import PartitionSpec as P


DH = 128
LANES = 128
NONE = -1000
VMEM = pl.BlockSpec(memory_space=pltpu.VMEM)
SMEM = pl.BlockSpec(memory_space=pltpu.SMEM)
SEND, KEEP, HOLD, NONE = 0, 5, 10, 15


def limit(mib):
    return pltpu.CompilerParams(vmem_limit_bytes=mib * 2**20)


def lookup(values, index):
    words = []
    for i in range(0, len(values), 8):
        word = sum(v << 4 * k for k, v in enumerate(values[i : i + 8]))
        words.append(word - 2**32 if word >= 2**31 else word)
    word = jnp.int32(words[0])
    for i in range(1, len(words)):
        word = jnp.where(index // 8 == i, jnp.int32(words[i]), word)
    return (word >> (4 * (index % 8))) & 15


def ring_order(n):
    return list(range(0, n, 2)) + list(range(n - 1, 0, -2))


def attention_kernel(n, span, group, sources, first, order_ref, docid_ref, docs_ref, q_ref, *rest):
    many = len(sources[0])
    split = 1 if first else 2
    kv_refs, rest = rest[: many * split], rest[many * split :]
    if first:
        top_ref, sum_ref, mix_ref, s_ref, m_ref, kv_ref, slot_ref, pos_ref = rest
    else:
        top_in, sum_in, mix_in, out_ref, s_ref, m_ref, kv_ref, slot_ref, pos_ref, *rest = rest
        sum_ref, mix_ref = rest
    base2 = math.log2(math.e) / math.sqrt(DH)
    mine = lax.axis_index("seq")
    dims = (((1,), (1,)), ((), ()))
    kposs = []
    for i in range(many):
        source = lookup([row[i] for row in sources], mine)
        kposs += [order_ref[2 * source], order_ref[2 * source + 1]]
    j = 0
    for ref in kv_refs:
        for at in range(0, ref.shape[0], span):
            kv_ref[j] = ref[at : at + span, :]
            j += 1
    ahead = lax.broadcasted_iota(jnp.int32, (span, span), 1) - lax.broadcasted_iota(
        jnp.int32, (span, span), 0
    )

    for part in range(2):
        rows = pl.ds(part * span, span)
        qpos = order_ref[2 * mine + part]
        qdoc = jnp.transpose(
            jnp.broadcast_to(docs_ref[pl.ds(qpos, 1), :], (span, span)).astype(jnp.float32)
        )
        qfirst = docid_ref[qpos * span]
        count = jnp.int32(0)
        for j, k in enumerate(kposs):
            slot_ref[count] = j
            pos_ref[count] = k
            live = (k <= qpos) & (docid_ref[k * span + span - 1] >= qfirst)
            count += live.astype(jnp.int32)
        slot_ref[count] = 0
        pos_ref[count] = qpos + 2 * n
        pairs = (count + 1) // 2
        m_ref[...] = jnp.full_like(m_ref, -1e30)

        def score(i, carry):
            bias, k = [], []
            for e in range(2):
                slot, kpos = slot_ref[2 * i + e], pos_ref[2 * i + e]
                kdoc = docs_ref[pl.ds(jnp.minimum(kpos, 2 * n - 1), 1), :].astype(jnp.float32)
                visible = (qdoc == kdoc) & (ahead <= (qpos - kpos) * span)
                bias.append(jnp.where(visible, 0.0, -1e30))
                k.append(kv_ref[slot, :, :DH])
            bias, k = jnp.concatenate(bias, axis=1), jnp.concatenate(k, axis=0)
            for h in range(group):
                q = q_ref[rows, h * DH : (h + 1) * DH]
                s = lax.dot_general(q, k, dims, preferred_element_type=jnp.float32) + bias
                at = slice(h * span, (h + 1) * span)
                s_ref[i, at, :] = s
                m_ref[at, :] = jnp.maximum(m_ref[at, :], jnp.maximum(s[:, :span], s[:, span:]))
            return carry

        lax.fori_loop(0, pairs, score, 0)
        largest = jnp.max(m_ref[...], axis=1, keepdims=True) * base2
        if first:
            m_ref[...] = jnp.broadcast_to(largest, m_ref.shape)
            top_ref[part] = m_ref[...]
            sum_ref[part] = jnp.zeros_like(m_ref)
            mix_ref[part] = jnp.zeros_like(m_ref)
        else:
            before = top_in[part]
            largest = jnp.maximum(before, largest)
            fade = jnp.exp2(before - largest)
            m_ref[...] = largest
            sum_ref[part] = sum_in[part] * fade
            mix_ref[part] = mix_in[part] * fade

        def mix(i, carry):
            v = jnp.concatenate([kv_ref[slot_ref[2 * i + e], :, DH:] for e in range(2)], axis=0)
            for h in range(group):
                at = slice(h * span, (h + 1) * span)
                top = m_ref[at, :]
                s = s_ref[i, at, :]
                p0 = jnp.exp2(s[:, :span] * base2 - top)
                p1 = jnp.exp2(s[:, span:] * base2 - top)
                sum_ref[part, at, :] += p0 + p1
                p = jnp.concatenate([p0.astype(jnp.bfloat16), p1.astype(jnp.bfloat16)], axis=1)
                mix_ref[part, at, :] += jnp.dot(p, v, preferred_element_type=jnp.float32)
            return carry

        lax.fori_loop(0, pairs, mix, 0)

        if not first:
            total = jnp.sum(sum_ref[part], axis=1, keepdims=True)
            attended = (mix_ref[part] / total).astype(jnp.bfloat16)
            for h in range(group):
                out_ref[rows, h * DH : (h + 1) * DH] = attended[h * span : (h + 1) * span]


def place():
    return lax.axis_index("seq") * lax.axis_size("head") + lax.axis_index("head")


def project_kernel(codes, moved, a_ref, b_ref, *rest):
    w_refs, rest = rest[: 2 * len(codes)], rest[2 * len(codes) :]
    if moved:
        held_ref, rest = rest[0], rest[1:]
    me = place()

    def put(at, c):
        for low, ref in zip((SEND, KEEP, HOLD), rest):

            @pl.when((at >= low) & (at < low + ref.shape[0]))
            def _():
                ref[at - low] = c

    for i, values in enumerate(moved):
        put(lookup(values, me), held_ref[i])
    for i, values in enumerate(codes):
        c = jnp.dot(a_ref[...], w_refs[2 * i][...], preferred_element_type=jnp.float32)
        c += jnp.dot(b_ref[...], w_refs[2 * i + 1][...], preferred_element_type=jnp.float32)
        put(lookup(values, me), c.astype(jnp.bfloat16))


def fold_kernel(codes, per, *rest):
    kept, came, (own_ref, send_ref) = rest[: len(codes)], rest[len(codes) : -2], rest[-2:]
    me = place()
    for r, slots in enumerate(codes):
        for i, values in enumerate(slots):
            at = lookup(values, me)

            @pl.when(at != NONE)
            def _():
                c = kept[r][i].astype(jnp.float32) + came[r][i].astype(jnp.float32)
                c = c.astype(jnp.bfloat16)

                @pl.when(at < per)
                def _():
                    own_ref[at] = c

                @pl.when(at >= per)
                def _():
                    send_ref[at - per] = c


def finish_kernel(own_ref, came_ref, out_ref):
    core = lax.axis_index("head") & 1
    per, _, half = own_ref.shape
    for part in range(per):
        for ref, side in ((own_ref, core), (came_ref, 1 - core)):
            start = pl.multiple_of((2 * part + side) * half, LANES)
            out_ref[:, pl.ds(start, half)] = ref[part]


def reduce_plan(n, heads, sources, rounds):
    per = n // heads
    devices = [(s, h) for s in range(n) for h in range(heads)]
    first = n // 2 - sum(len(places) for places in rounds[1:])
    caps = [max(1, first)] + [len(places) for places in rounds[1:]]
    turns = {}
    for s in range(n):
        for owners in (0, 2):
            room = list(caps)
            for r, places in enumerate(rounds):
                for p in places:
                    if (sources[s][p] // per) & 2 == owners:
                        at = next(k for k in range(r, len(caps)) if room[k])
                        room[at] -= 1
                        turns[s, p] = at
    plan = []
    held = {d: [] for d in devices}
    for r, places in enumerate(rounds):
        codes, moved = [[] for _ in places], [[] for _ in range(max(map(len, held.values())))]
        kept, later = {d: [] for d in devices}, {d: [] for d in devices}
        for s, h in devices:
            sent = 0
            jobs = [(moved[i], p) for i, p in enumerate(held[s, h])]
            jobs += [(codes[i], p) for i, p in enumerate(places)]
            for row, p in jobs:
                block = sources[s][p]
                away = (block // per) ^ h
                if turns[s, p] > r:
                    row.append(HOLD + len(later[s, h]))
                    later[s, h].append(p)
                elif away & 2:
                    row.append(SEND + sent)
                    sent += 1
                else:
                    row.append(KEEP + len(kept[s, h]))
                    kept[s, h].append(block % per + per * (away & 1))
            for row in moved[len(held[s, h]) :]:
                row.append(NONE)
        held = later
        ends = [[v[i] if i < len(v) else NONE for v in kept.values()] for i in range(caps[r])]
        plan.append((codes, moved, caps[r], max(map(len, held.values())), ends))
    return plan


def ring_device(n, heads, queries, keys, values, doc_ids, span_order, out_weight):
    tok_rows = queries.shape[0]
    span = tok_rows // 2
    group = queries.shape[1] // DH
    width = out_weight.shape[1]
    per = n // heads
    hops = n // 2
    ring = ring_order(n)
    where = {s: i for i, s in enumerate(ring)}
    sources = []
    for s in range(n):
        row = [s]
        for hop in range(1, hops):
            row += [ring[(where[s] - hop) % n], ring[(where[s] + hop) % n]]
        sources.append(row + [ring[(where[s] + hops) % n]])

    def gather(pieces):
        def move(way, x):
            step = 1 if way == "up" else -1
            pairs = [(ring[p], ring[(p + step) % n]) for p in range(n)]
            return lax.ppermute(x, "seq", pairs)

        ups, downs = list(pieces), list(pieces)
        got = [list(pieces)]
        for _ in range(1, hops):
            for i in range(len(pieces)):
                ups[i] = move("up", ups[i])
                downs[i] = move("dn", downs[i])
            got += [list(ups), list(downs)]
        if len(pieces) == 1:
            rows = pieces[0].shape[0] // 2
            ups, downs = [ups[0][:rows], None], [None, downs[0][rows:]]
        got.append([move("up", ups[0]), move("dn", downs[1])])
        return got

    half = width // 2
    both = jnp.concatenate([keys, values], axis=1)
    left, right, both = lax.optimization_barrier(
        (out_weight[:, :half], out_weight[:, half:], both)
    )
    kv = gather([both])
    first = (lax.axis_index("head") & 1) == 0
    mine, other = jnp.where(first, left, right), jnp.where(first, right, left)
    beside = [(h, h ^ 1) for h in range(heads)]
    other = lax.ppermute(other, "head", beside)
    w = gather([mine, other])

    def attend(stage, slots, state, out_shape):
        first = stage == 0
        block = pltpu.VMEM((group * span, span), jnp.float32)
        states = pltpu.VMEM((2, group * span, span), jnp.float32)
        share = 2 * len(slots) * group * tok_rows * tok_rows
        args = [queries] + [piece for i in slots for piece in kv[i]] + state
        return pl.pallas_call(
            functools.partial(
                attention_kernel,
                n,
                span,
                group,
                [[row[i] for i in slots] for row in sources],
                first,
            ),
            out_shape=out_shape,
            in_specs=[SMEM, SMEM] + [VMEM] * (1 + len(args)),
            out_specs=jax.tree.map(lambda _: VMEM, out_shape),
            scratch_shapes=[
                pltpu.VMEM((len(slots), group * span, 2 * span), jnp.float32),
                block,
                pltpu.VMEM((2 * len(slots), span, 2 * DH), jnp.bfloat16),
                pltpu.SMEM((2 * len(slots) + 1,), jnp.int32),
                pltpu.SMEM((2 * len(slots) + 1,), jnp.int32),
            ]
            + ([] if first else [states, states]),
            compiler_params=limit(16),
            cost_estimate=pl.CostEstimate(
                flops=2 * share * DH,
                bytes_accessed=len(slots) * tok_rows * 4 * DH,
                transcendentals=share,
            ),
            name="attend",
        )(span_order, doc_ids, doc_ids.reshape(-1, span), *args)

    memory = jax.ShapeDtypeStruct((2, group * span, span), jnp.float32)
    state = attend(0, range(n - 1), [], (memory,) * 3)
    attended = attend(
        1, [n - 1], list(state), jax.ShapeDtypeStruct((tok_rows, group * DH), jnp.bfloat16)
    )
    paired = lax.ppermute(attended, "head", beside)

    def block(count):
        return jax.ShapeDtypeStruct((count, tok_rows, half), jnp.bfloat16)

    rounds = [list(range(n - 3)), [n - 3, n - 2], [n - 1]]
    across = [(h, h ^ 2) for h in range(heads)]
    kept, came, ends, held = [], [], [], []
    for r, (codes, moved, count, hold, end) in enumerate(
        reduce_plan(n, heads, sources, rounds)
    ):
        pieces = [piece for p in rounds[r] for piece in w[p]]
        outs = (block(count), block(count)) + ((block(hold),) if hold else ())
        send, keep, *rest = pl.pallas_call(
            functools.partial(project_kernel, codes, moved),
            out_shape=outs,
            in_specs=[VMEM] * (2 + len(pieces) + len(held)),
            out_specs=(VMEM,) * len(outs),
            compiler_params=limit(8),
            cost_estimate=pl.CostEstimate(
                flops=2 * tok_rows * group * DH * half * len(pieces),
                bytes_accessed=2 * group * DH * half * len(pieces),
                transcendentals=0,
            ),
            name="project",
        )(attended, paired, *pieces, *held)
        came.append(lax.ppermute(send, "head", across))
        held = rest
        kept.append(keep)
        ends.append(end)

    own, send = pl.pallas_call(
        functools.partial(fold_kernel, ends, per),
        out_shape=(block(per), block(per)),
        in_specs=[VMEM] * (2 * len(ends)),
        out_specs=(VMEM, VMEM),
        compiler_params=limit(8),
        name="fold",
    )(*kept, *came)
    joined = lax.ppermute(send, "head", beside)
    return pl.pallas_call(
        finish_kernel,
        out_shape=jax.ShapeDtypeStruct((tok_rows, per * width), jnp.bfloat16),
        in_specs=[VMEM, VMEM],
        out_specs=VMEM,
        compiler_params=limit(8),
        name="finish",
    )(own, joined)


def on_device(queries, keys, values, doc_ids, span_order, out_weight):
    tok_rows = queries.shape[0]
    span = tok_rows // 2
    local_heads = queries.shape[1] // DH
    local_kv = keys.shape[1] // DH
    group_size = local_heads // local_kv
    n_blocks = span_order.shape[0]
    scale = 1.0 / math.sqrt(DH)
    mine = lax.axis_index("seq")
    own_blocks = lax.dynamic_slice_in_dim(span_order, 2 * mine, 2, 0)
    local_rows = jnp.arange(tok_rows, dtype=jnp.int32)
    qpos = jnp.where(local_rows < span, own_blocks[0], own_blocks[1]) * span + local_rows % span
    qdoc = jnp.take(doc_ids, qpos)
    q_heads = queries.reshape(tok_rows, local_kv, group_size, DH)

    def update(state, kblk, vblk, kpos, kdoc):
        largest, total, summed = state
        count = kblk.shape[0]
        k_heads = kblk.reshape(count, local_kv, DH)
        v_heads = vblk.reshape(count, local_kv, DH)
        scores = (
            jnp.einsum("qhgd,khd->hgqk", q_heads, k_heads, preferred_element_type=jnp.float32)
            * scale
        )
        visible = (qdoc[:, None] == kdoc[None, :]) & (kpos[None, :] <= qpos[:, None])
        masked = jnp.where(visible, scores, jnp.float32(-1e30))
        new_largest = jnp.maximum(largest, jnp.max(masked, axis=-1))
        factor = jnp.exp(largest - new_largest)
        weights = jnp.where(visible, jnp.exp(masked - new_largest[..., None]), jnp.float32(0.0))
        total = total * factor + jnp.sum(weights, axis=-1)
        weights_b = weights.astype(jnp.bfloat16)
        added = jnp.einsum("hgqk,khd->qhgd", weights_b, v_heads, preferred_element_type=jnp.float32)
        summed = summed * jnp.transpose(factor, (2, 0, 1))[..., None] + added
        return (new_largest, total, summed)

    initial = (
        jnp.full((local_kv, group_size, tok_rows), -1e30, jnp.float32),
        jnp.zeros((local_kv, group_size, tok_rows), jnp.float32),
        jnp.zeros((tok_rows, local_kv, group_size, DH), jnp.float32),
    )
    state = initial
    kpiece = lax.all_gather(keys, "seq", axis=0, tiled=True)
    vpiece = lax.all_gather(values, "seq", axis=0, tiled=True)
    count = kpiece.shape[0]
    width = math.gcd(count, 1024)
    steps = count // width
    rows = jnp.arange(count, dtype=jnp.int32)
    match = (rows // span)[:, None] == jnp.arange(n_blocks, dtype=jnp.int32)[None, :]
    owner = jnp.sum(jnp.where(match, span_order[None, :], 0), axis=1)
    kpos = owner * span + rows % span
    kdoc = jnp.take(doc_ids, kpos)
    kparts = kpiece.reshape(steps, width, kpiece.shape[1])
    vparts = vpiece.reshape(steps, width, vpiece.shape[1])

    def one_step(carry, items):
        kblk, vblk, pblk, dblk = items
        carry = update(carry, kblk, vblk, pblk, dblk)
        return (carry, None)

    state, _ = lax.scan(
        one_step, state, (kparts, vparts, kpos.reshape(steps, width), kdoc.reshape(steps, width))
    )
    _, total, summed = state
    attended = (summed / jnp.transpose(total, (2, 0, 1))[..., None]).astype(jnp.bfloat16)
    attended = attended.reshape(tok_rows, local_heads * DH)
    partial_out = jnp.dot(
        attended,
        lax.all_gather(out_weight, "seq", axis=1, tiled=True),
        preferred_element_type=jnp.float32,
    )
    return lax.psum_scatter(
        partial_out.astype(jnp.bfloat16), "head", scatter_dimension=1, tiled=True
    )


def solution(mesh):
    n, heads = mesh.shape["seq"], mesh.shape["head"]

    def on_each(queries, keys, values, doc_ids, span_order, out_weight):
        span = queries.shape[0] // 2
        ring = (
            4 <= n <= 16
            and n % 2 == 0
            and n % heads == 0
            and heads == 4
            and keys.shape[1] == DH
            and span % LANES == 0
            and out_weight.shape[1] % (2 * LANES) == 0
        )
        args = (queries, keys, values, doc_ids, span_order, out_weight)
        if not ring:
            return on_device(*args)
        return ring_device(n, heads, *args)

    return jax.shard_map(
        on_each,
        mesh=mesh,
        in_specs=(P("seq", "head"), P("seq", "head"), P("seq", "head"), P(), P(), P("head", "seq")),
        out_specs=P("seq", "head"),
        check_vma=False,
    )
```

```python
import functools
import math

import jax
import jax.numpy as jnp
from jax import lax
from jax.experimental import pallas as pl
from jax.experimental.pallas import tpu as pltpu
from jax.sharding import PartitionSpec as P


DH = 128
LANES = 128
NONE = -1000
VMEM = pl.BlockSpec(memory_space=pltpu.VMEM)
SMEM = pl.BlockSpec(memory_space=pltpu.SMEM)
HBM = pl.BlockSpec(memory_space=pltpu.HBM)
SEND, KEEP, HOLD, NONE = 0, 5, 10, 15


def limit(mib):
    return pltpu.CompilerParams(vmem_limit_bytes=mib * 2**20)


def lookup(values, index):
    words = []
    for i in range(0, len(values), 8):
        word = sum(v << 4 * k for k, v in enumerate(values[i : i + 8]))
        words.append(word - 2**32 if word >= 2**31 else word)
    word = jnp.int32(words[0])
    for i in range(1, len(words)):
        word = jnp.where(index // 8 == i, jnp.int32(words[i]), word)
    return (word >> (4 * (index % 8))) & 15


def ring_order(n):
    return list(range(0, n, 2)) + list(range(n - 1, 0, -2))


def attention_kernel(n, span, group, sources, first, order_ref, docid_ref, docs_ref, q_ref, *rest):
    many = len(sources[0])
    split = 1 if first else 2
    kv_refs, rest = rest[: many * split], rest[many * split :]
    if first:
        top_ref, sum_ref, mix_ref, s_ref, m_ref, kv_ref, slot_ref, pos_ref = rest
    else:
        top_in, sum_in, mix_in, out_ref, s_ref, m_ref, kv_ref, slot_ref, pos_ref, *rest = rest
        sum_ref, mix_ref = rest
    base2 = math.log2(math.e) / math.sqrt(DH)
    mine = lax.axis_index("seq")
    dims = (((1,), (1,)), ((), ()))
    kposs = []
    for i in range(many):
        source = lookup([row[i] for row in sources], mine)
        kposs += [order_ref[2 * source], order_ref[2 * source + 1]]
    j = 0
    for ref in kv_refs:
        for at in range(0, ref.shape[0], span):
            kv_ref[j] = ref[at : at + span, :]
            j += 1
    ahead = lax.broadcasted_iota(jnp.int32, (span, span), 1) - lax.broadcasted_iota(
        jnp.int32, (span, span), 0
    )

    for part in range(2):
        rows = pl.ds(part * span, span)
        qpos = order_ref[2 * mine + part]
        qdoc = jnp.transpose(
            jnp.broadcast_to(docs_ref[pl.ds(qpos, 1), :], (span, span)).astype(jnp.float32)
        )
        qfirst = docid_ref[qpos * span]
        count = jnp.int32(0)
        for j, k in enumerate(kposs):
            slot_ref[count] = j
            pos_ref[count] = k
            live = (k <= qpos) & (docid_ref[k * span + span - 1] >= qfirst)
            count += live.astype(jnp.int32)
        slot_ref[count] = 0
        pos_ref[count] = qpos + 2 * n
        pairs = (count + 1) // 2
        m_ref[...] = jnp.full_like(m_ref, -1e30)

        def score(i, carry):
            bias, k = [], []
            for e in range(2):
                slot, kpos = slot_ref[2 * i + e], pos_ref[2 * i + e]
                kdoc = docs_ref[pl.ds(jnp.minimum(kpos, 2 * n - 1), 1), :].astype(jnp.float32)
                visible = (qdoc == kdoc) & (ahead <= (qpos - kpos) * span)
                bias.append(jnp.where(visible, 0.0, -1e30))
                k.append(kv_ref[slot, :, :DH])
            bias, k = jnp.concatenate(bias, axis=1), jnp.concatenate(k, axis=0)
            for h in range(group):
                q = q_ref[rows, h * DH : (h + 1) * DH]
                s = lax.dot_general(q, k, dims, preferred_element_type=jnp.float32) + bias
                at = slice(h * span, (h + 1) * span)
                s_ref[i, at, :] = s
                m_ref[at, :] = jnp.maximum(m_ref[at, :], jnp.maximum(s[:, :span], s[:, span:]))
            return carry

        lax.fori_loop(0, pairs, score, 0)
        largest = jnp.max(m_ref[...], axis=1, keepdims=True) * base2
        if first:
            m_ref[...] = jnp.broadcast_to(largest, m_ref.shape)
            top_ref[part] = m_ref[...]
            sum_ref[part] = jnp.zeros_like(m_ref)
            mix_ref[part] = jnp.zeros_like(m_ref)
        else:
            before = top_in[part]
            largest = jnp.maximum(before, largest)
            fade = jnp.exp2(before - largest)
            m_ref[...] = largest
            sum_ref[part] = sum_in[part] * fade
            mix_ref[part] = mix_in[part] * fade

        def mix(i, carry):
            v = jnp.concatenate([kv_ref[slot_ref[2 * i + e], :, DH:] for e in range(2)], axis=0)
            for h in range(group):
                at = slice(h * span, (h + 1) * span)
                top = m_ref[at, :]
                s = s_ref[i, at, :]
                p0 = jnp.exp2(s[:, :span] * base2 - top)
                p1 = jnp.exp2(s[:, span:] * base2 - top)
                sum_ref[part, at, :] += p0 + p1
                p = jnp.concatenate([p0.astype(jnp.bfloat16), p1.astype(jnp.bfloat16)], axis=1)
                mix_ref[part, at, :] += jnp.dot(p, v, preferred_element_type=jnp.float32)
            return carry

        lax.fori_loop(0, pairs, mix, 0)

        if not first:
            total = jnp.sum(sum_ref[part], axis=1, keepdims=True)
            attended = (mix_ref[part] / total).astype(jnp.bfloat16)
            for h in range(group):
                out_ref[rows, h * DH : (h + 1) * DH] = attended[h * span : (h + 1) * span]


def place():
    return lax.axis_index("seq") * lax.axis_size("head") + lax.axis_index("head")


def project_kernel(codes, moved, a_ref, b_ref, *rest):
    w_refs, rest = rest[: 2 * len(codes)], rest[2 * len(codes) :]
    if moved:
        held_ref, rest = rest[0], rest[1:]
    me = place()

    def put(at, c):
        for low, ref in zip((SEND, KEEP, HOLD), rest):

            @pl.when((at >= low) & (at < low + ref.shape[0]))
            def _():
                ref[at - low] = c

    for i, values in enumerate(moved):
        put(lookup(values, me), held_ref[i])
    for i, values in enumerate(codes):
        c = jnp.dot(a_ref[...], w_refs[2 * i][...], preferred_element_type=jnp.float32)
        c += jnp.dot(b_ref[...], w_refs[2 * i + 1][...], preferred_element_type=jnp.float32)
        put(lookup(values, me), c.astype(jnp.bfloat16))


def fold_kernel(codes, spans, per, *rest):
    kept, came, (own_ref, send_ref) = rest[: len(codes)], rest[len(codes) : -2], rest[-2:]
    me = place()
    for r, slots in enumerate(codes):
        cols = slice(*spans[r])
        for i, values in enumerate(slots):
            at = lookup(values, me)

            @pl.when(at != NONE)
            def _():
                c = kept[r][i].astype(jnp.float32) + came[r][i].astype(jnp.float32)
                c = c.astype(jnp.bfloat16)

                @pl.when(at < per)
                def _():
                    own_ref[at, :, cols] = c

                @pl.when(at >= per)
                def _():
                    send_ref[at - per, :, cols] = c


def finish_kernel(side, part_ref, *rest):
    out_ref, sem = rest[-2:]
    per, _, half = part_ref.shape
    core = (lax.axis_index("head") & 1) ^ side
    copies = []
    for part in range(per):
        start = pl.multiple_of((2 * part + core) * half, LANES)
        columns = out_ref.at[:, pl.ds(start, half)]
        copies.append(pltpu.make_async_copy(part_ref.at[part], columns, sem.at[part]))
        copies[-1].start()
    for copy in copies:
        copy.wait()


def reduce_plan(n, heads, sources, rounds):
    per = n // heads
    devices = [(s, h) for s in range(n) for h in range(heads)]
    caps = [max(1, n // 2 - len(rounds[1]))] + [len(places) for places in rounds[1:]]
    sources = [row + row[-1:] for row in sources]
    turns = {}
    for s in range(n):
        for owners in (0, 2):
            room = list(caps)
            for r, places in enumerate(rounds):
                for p in places:
                    if (sources[s][p] // per) & 2 == owners:
                        at = next(k for k in (r, *range(r + 1, 2)) if room[k])
                        room[at] -= 1
                        turns[s, p] = at
    plan = []
    held = {d: [] for d in devices}
    for r, places in enumerate(rounds):
        codes, moved = [[] for _ in places], [[] for _ in range(max(map(len, held.values())))]
        kept, later = {d: [] for d in devices}, {d: [] for d in devices}
        for s, h in devices:
            sent = 0
            jobs = [(moved[i], p) for i, p in enumerate(held[s, h])]
            jobs += [(codes[i], p) for i, p in enumerate(places)]
            for row, p in jobs:
                block = sources[s][p]
                away = (block // per) ^ h
                if turns[s, p] > r:
                    row.append(HOLD + len(later[s, h]))
                    later[s, h].append(p)
                elif away & 2:
                    row.append(SEND + sent)
                    sent += 1
                else:
                    row.append(KEEP + len(kept[s, h]))
                    kept[s, h].append(block % per + per * (away & 1))
            for row in moved[len(held[s, h]) :]:
                row.append(NONE)
        held = later
        ends = [[v[i] if i < len(v) else NONE for v in kept.values()] for i in range(caps[r])]
        plan.append((codes, moved, caps[r], max(map(len, held.values())), ends))
    return plan


def ring_device(n, heads, queries, keys, values, doc_ids, span_order, out_weight):
    tok_rows = queries.shape[0]
    span = tok_rows // 2
    group = queries.shape[1] // DH
    width = out_weight.shape[1]
    per = n // heads
    hops = n // 2
    ring = ring_order(n)
    where = {s: i for i, s in enumerate(ring)}
    sources = []
    for s in range(n):
        row = [s]
        for hop in range(1, hops):
            row += [ring[(where[s] - hop) % n], ring[(where[s] + hop) % n]]
        sources.append(row + [ring[(where[s] + hops) % n]])

    def gather(pieces):
        def move(way, x):
            step = 1 if way == "up" else -1
            pairs = [(ring[p], ring[(p + step) % n]) for p in range(n)]
            return lax.ppermute(x, "seq", pairs)

        ups, downs = list(pieces), list(pieces)
        got = [list(pieces)]
        for _ in range(1, hops):
            for i in range(len(pieces)):
                ups[i] = move("up", ups[i])
                downs[i] = move("dn", downs[i])
            got += [list(ups), list(downs)]
        if len(pieces) == 1:
            rows = pieces[0].shape[0] // 2
            parts = [(ups[0][:rows], downs[0][rows:])]
        else:
            cols = pieces[0].shape[1] // 2
            parts = [(ups[0][:, :cols], downs[1][:, :cols]), (ups[0][:, cols:], downs[1][:, cols:])]
        for up, down in parts:
            got.append([move("up", up), move("dn", down)])
        return got

    half = width // 2
    both = jnp.concatenate([keys, values], axis=1)
    left, right, both = lax.optimization_barrier(
        (out_weight[:, :half], out_weight[:, half:], both)
    )
    kv = gather([both])
    first = (lax.axis_index("head") & 1) == 0
    mine, other = jnp.where(first, left, right), jnp.where(first, right, left)
    beside = [(h, h ^ 1) for h in range(heads)]
    other = lax.ppermute(other, "head", beside)
    w = gather([mine, other])

    def attend(stage, slots, state, out_shape):
        first = stage == 0
        block = pltpu.VMEM((group * span, span), jnp.float32)
        states = pltpu.VMEM((2, group * span, span), jnp.float32)
        share = 2 * len(slots) * group * tok_rows * tok_rows
        args = [queries] + [piece for i in slots for piece in kv[i]] + state
        return pl.pallas_call(
            functools.partial(
                attention_kernel,
                n,
                span,
                group,
                [[row[i] for i in slots] for row in sources],
                first,
            ),
            out_shape=out_shape,
            in_specs=[SMEM, SMEM] + [VMEM] * (1 + len(args)),
            out_specs=jax.tree.map(lambda _: VMEM, out_shape),
            scratch_shapes=[
                pltpu.VMEM((len(slots), group * span, 2 * span), jnp.float32),
                block,
                pltpu.VMEM((2 * len(slots), span, 2 * DH), jnp.bfloat16),
                pltpu.SMEM((2 * len(slots) + 1,), jnp.int32),
                pltpu.SMEM((2 * len(slots) + 1,), jnp.int32),
            ]
            + ([] if first else [states, states]),
            compiler_params=limit(16),
            cost_estimate=pl.CostEstimate(
                flops=2 * share * DH,
                bytes_accessed=len(slots) * tok_rows * 4 * DH,
                transcendentals=share,
            ),
            name="attend",
        )(span_order, doc_ids, doc_ids.reshape(-1, span), *args)

    memory = jax.ShapeDtypeStruct((2, group * span, span), jnp.float32)
    state = attend(0, range(n - 1), [], (memory,) * 3)
    attended = attend(
        1, [n - 1], list(state), jax.ShapeDtypeStruct((tok_rows, group * DH), jnp.bfloat16)
    )
    paired = lax.ppermute(attended, "head", beside)

    def block(count, cols):
        return jax.ShapeDtypeStruct((count, tok_rows, cols), jnp.bfloat16)

    rounds = [list(range(n - 3)), [n - 3, n - 2], [n - 1], [n]]
    quarter = half // 2
    spans = [(0, half), (0, half), (0, quarter), (quarter, half)]
    across = [(h, h ^ 2) for h in range(heads)]
    kept, came, ends, held = [], [], [], []
    for r, (codes, moved, count, hold, end) in enumerate(
        reduce_plan(n, heads, sources, rounds)
    ):
        pieces = [piece for p in rounds[r] for piece in w[p]]
        cols = spans[r][1] - spans[r][0]
        outs = (block(count, cols),) * 2 + ((block(hold, cols),) if hold else ())
        send, keep, *rest = pl.pallas_call(
            functools.partial(project_kernel, codes, moved),
            out_shape=outs,
            in_specs=[VMEM] * (2 + len(pieces) + len(held)),
            out_specs=(VMEM,) * len(outs),
            compiler_params=limit(8),
            cost_estimate=pl.CostEstimate(
                flops=2 * tok_rows * group * DH * cols * len(pieces),
                bytes_accessed=2 * group * DH * cols * len(pieces),
                transcendentals=0,
            ),
            name="project",
        )(attended, paired, *pieces, *held)
        came.append(lax.ppermute(send, "head", across))
        held = rest
        kept.append(keep)
        ends.append(end)

    own, send = pl.pallas_call(
        functools.partial(fold_kernel, ends, spans, per),
        out_shape=(block(per, half),) * 2,
        in_specs=[VMEM] * (2 * len(ends)),
        out_specs=(VMEM, VMEM),
        compiler_params=limit(8),
        name="fold",
    )(*kept, *came)
    joined = lax.ppermute(send, "head", beside)

    def finish(side, part, *out):
        return pl.pallas_call(
            functools.partial(finish_kernel, side),
            out_shape=jax.ShapeDtypeStruct((tok_rows, per * width), jnp.bfloat16),
            in_specs=[VMEM] + [HBM] * len(out),
            out_specs=HBM,
            input_output_aliases={1: 0} if out else {},
            scratch_shapes=[pltpu.SemaphoreType.DMA((per,))],
            compiler_params=limit(4),
            name="finish",
        )(part, *out)

    return finish(1, joined, finish(0, own))


def on_device(queries, keys, values, doc_ids, span_order, out_weight):
    tok_rows = queries.shape[0]
    span = tok_rows // 2
    local_heads = queries.shape[1] // DH
    local_kv = keys.shape[1] // DH
    group_size = local_heads // local_kv
    n_blocks = span_order.shape[0]
    scale = 1.0 / math.sqrt(DH)
    mine = lax.axis_index("seq")
    own_blocks = lax.dynamic_slice_in_dim(span_order, 2 * mine, 2, 0)
    local_rows = jnp.arange(tok_rows, dtype=jnp.int32)
    qpos = jnp.where(local_rows < span, own_blocks[0], own_blocks[1]) * span + local_rows % span
    qdoc = jnp.take(doc_ids, qpos)
    q_heads = queries.reshape(tok_rows, local_kv, group_size, DH)

    def update(state, kblk, vblk, kpos, kdoc):
        largest, total, summed = state
        count = kblk.shape[0]
        k_heads = kblk.reshape(count, local_kv, DH)
        v_heads = vblk.reshape(count, local_kv, DH)
        scores = (
            jnp.einsum("qhgd,khd->hgqk", q_heads, k_heads, preferred_element_type=jnp.float32)
            * scale
        )
        visible = (qdoc[:, None] == kdoc[None, :]) & (kpos[None, :] <= qpos[:, None])
        masked = jnp.where(visible, scores, jnp.float32(-1e30))
        new_largest = jnp.maximum(largest, jnp.max(masked, axis=-1))
        factor = jnp.exp(largest - new_largest)
        weights = jnp.where(visible, jnp.exp(masked - new_largest[..., None]), jnp.float32(0.0))
        total = total * factor + jnp.sum(weights, axis=-1)
        weights_b = weights.astype(jnp.bfloat16)
        added = jnp.einsum("hgqk,khd->qhgd", weights_b, v_heads, preferred_element_type=jnp.float32)
        summed = summed * jnp.transpose(factor, (2, 0, 1))[..., None] + added
        return (new_largest, total, summed)

    initial = (
        jnp.full((local_kv, group_size, tok_rows), -1e30, jnp.float32),
        jnp.zeros((local_kv, group_size, tok_rows), jnp.float32),
        jnp.zeros((tok_rows, local_kv, group_size, DH), jnp.float32),
    )
    state = initial
    kpiece = lax.all_gather(keys, "seq", axis=0, tiled=True)
    vpiece = lax.all_gather(values, "seq", axis=0, tiled=True)
    count = kpiece.shape[0]
    width = math.gcd(count, 1024)
    steps = count // width
    rows = jnp.arange(count, dtype=jnp.int32)
    match = (rows // span)[:, None] == jnp.arange(n_blocks, dtype=jnp.int32)[None, :]
    owner = jnp.sum(jnp.where(match, span_order[None, :], 0), axis=1)
    kpos = owner * span + rows % span
    kdoc = jnp.take(doc_ids, kpos)
    kparts = kpiece.reshape(steps, width, kpiece.shape[1])
    vparts = vpiece.reshape(steps, width, vpiece.shape[1])

    def one_step(carry, items):
        kblk, vblk, pblk, dblk = items
        carry = update(carry, kblk, vblk, pblk, dblk)
        return (carry, None)

    state, _ = lax.scan(
        one_step, state, (kparts, vparts, kpos.reshape(steps, width), kdoc.reshape(steps, width))
    )
    _, total, summed = state
    attended = (summed / jnp.transpose(total, (2, 0, 1))[..., None]).astype(jnp.bfloat16)
    attended = attended.reshape(tok_rows, local_heads * DH)
    partial_out = jnp.dot(
        attended,
        lax.all_gather(out_weight, "seq", axis=1, tiled=True),
        preferred_element_type=jnp.float32,
    )
    return lax.psum_scatter(
        partial_out.astype(jnp.bfloat16), "head", scatter_dimension=1, tiled=True
    )


def solution(mesh):
    n, heads = mesh.shape["seq"], mesh.shape["head"]

    def on_each(queries, keys, values, doc_ids, span_order, out_weight):
        span = queries.shape[0] // 2
        ring = (
            4 <= n <= 16
            and n % 2 == 0
            and n % heads == 0
            and heads == 4
            and keys.shape[1] == DH
            and span % LANES == 0
            and out_weight.shape[1] % (4 * LANES) == 0
        )
        args = (queries, keys, values, doc_ids, span_order, out_weight)
        if not ring:
            return on_device(*args)
        return ring_device(n, heads, *args)

    return jax.shard_map(
        on_each,
        mesh=mesh,
        in_specs=(P("seq", "head"), P("seq", "head"), P("seq", "head"), P(), P(), P("head", "seq")),
        out_specs=P("seq", "head"),
        check_vma=False,
    )
```

```python
import functools
import math

import jax
import jax.numpy as jnp
from jax import lax
from jax.experimental import pallas as pl
from jax.experimental.pallas import tpu as pltpu
from jax.sharding import PartitionSpec as P


DH = 128
LANES = 128
NONE = -1000
VMEM = pl.BlockSpec(memory_space=pltpu.VMEM)
SMEM = pl.BlockSpec(memory_space=pltpu.SMEM)
HBM = pl.BlockSpec(memory_space=pltpu.HBM)
SEND, KEEP, HOLD, NONE = 0, 5, 10, 15


def limit(mib):
    return pltpu.CompilerParams(vmem_limit_bytes=mib * 2**20)


def lookup(values, index):
    words = []
    for i in range(0, len(values), 8):
        word = sum(v << 4 * k for k, v in enumerate(values[i : i + 8]))
        words.append(word - 2**32 if word >= 2**31 else word)
    word = jnp.int32(words[0])
    for i in range(1, len(words)):
        word = jnp.where(index // 8 == i, jnp.int32(words[i]), word)
    return (word >> (4 * (index % 8))) & 15


def ring_order(n):
    return list(range(0, n, 2)) + list(range(n - 1, 0, -2))


def attention_kernel(n, span, group, sources, first, order_ref, docid_ref, docs_ref, q_ref, *rest):
    many = len(sources[0])
    split = 1 if first else 2
    kv_refs, rest = rest[: many * split], rest[many * split :]
    if first:
        top_ref, sum_ref, mix_ref, s_ref, m_ref, kv_ref, slot_ref, pos_ref = rest
    else:
        top_in, sum_in, mix_in, out_ref, s_ref, m_ref, kv_ref, slot_ref, pos_ref, *rest = rest
        sum_ref, mix_ref = rest
    base2 = math.log2(math.e) / math.sqrt(DH)
    mine = lax.axis_index("seq")
    dims = (((1,), (1,)), ((), ()))
    kposs = []
    for i in range(many):
        source = lookup([row[i] for row in sources], mine)
        kposs += [order_ref[2 * source], order_ref[2 * source + 1]]
    j = 0
    for ref in kv_refs:
        for at in range(0, ref.shape[0], span):
            kv_ref[j] = ref[at : at + span, :]
            j += 1
    ahead = lax.broadcasted_iota(jnp.int32, (span, span), 1) - lax.broadcasted_iota(
        jnp.int32, (span, span), 0
    )

    for part in range(2):
        rows = pl.ds(part * span, span)
        qpos = order_ref[2 * mine + part]
        qdoc = jnp.transpose(
            jnp.broadcast_to(docs_ref[pl.ds(qpos, 1), :], (span, span)).astype(jnp.float32)
        )
        qfirst = docid_ref[qpos * span]
        count = jnp.int32(0)
        for j, k in enumerate(kposs):
            slot_ref[count] = j
            pos_ref[count] = k
            live = (k <= qpos) & (docid_ref[k * span + span - 1] >= qfirst)
            count += live.astype(jnp.int32)
        slot_ref[count] = 0
        pos_ref[count] = qpos + 2 * n
        pairs = (count + 1) // 2
        m_ref[...] = jnp.full_like(m_ref, -1e30)

        def score(i, carry):
            bias, k = [], []
            for e in range(2):
                slot, kpos = slot_ref[2 * i + e], pos_ref[2 * i + e]
                kdoc = docs_ref[pl.ds(jnp.minimum(kpos, 2 * n - 1), 1), :].astype(jnp.float32)
                visible = (qdoc == kdoc) & (ahead <= (qpos - kpos) * span)
                bias.append(jnp.where(visible, 0.0, -1e30))
                k.append(kv_ref[slot, :, :DH])
            bias, k = jnp.concatenate(bias, axis=1), jnp.concatenate(k, axis=0)
            for h in range(group):
                q = q_ref[rows, h * DH : (h + 1) * DH]
                s = lax.dot_general(q, k, dims, preferred_element_type=jnp.float32) + bias
                at = slice(h * span, (h + 1) * span)
                s_ref[i, at, :] = s
                m_ref[at, :] = jnp.maximum(m_ref[at, :], jnp.maximum(s[:, :span], s[:, span:]))
            return carry

        lax.fori_loop(0, pairs, score, 0)
        largest = jnp.max(m_ref[...], axis=1, keepdims=True) * base2
        if first:
            m_ref[...] = jnp.broadcast_to(largest, m_ref.shape)
            top_ref[part] = m_ref[...]
            sum_ref[part] = jnp.zeros_like(m_ref)
            mix_ref[part] = jnp.zeros_like(m_ref)
        else:
            before = top_in[part]
            largest = jnp.maximum(before, largest)
            fade = jnp.exp2(before - largest)
            m_ref[...] = largest
            sum_ref[part] = sum_in[part] * fade
            mix_ref[part] = mix_in[part] * fade

        def mix(i, carry):
            v = jnp.concatenate([kv_ref[slot_ref[2 * i + e], :, DH:] for e in range(2)], axis=0)
            for h in range(group):
                at = slice(h * span, (h + 1) * span)
                top = m_ref[at, :]
                s = s_ref[i, at, :]
                p0 = jnp.exp2(s[:, :span] * base2 - top)
                p1 = jnp.exp2(s[:, span:] * base2 - top)
                sum_ref[part, at, :] += p0 + p1
                p = jnp.concatenate([p0.astype(jnp.bfloat16), p1.astype(jnp.bfloat16)], axis=1)
                mix_ref[part, at, :] += jnp.dot(p, v, preferred_element_type=jnp.float32)
            return carry

        lax.fori_loop(0, pairs, mix, 0)

        if not first:
            total = jnp.sum(sum_ref[part], axis=1, keepdims=True)
            attended = (mix_ref[part] / total).astype(jnp.bfloat16)
            for h in range(group):
                out_ref[rows, h * DH : (h + 1) * DH] = attended[h * span : (h + 1) * span]


def place():
    return lax.axis_index("seq") * lax.axis_size("head") + lax.axis_index("head")


def early_kernel(a_ref, b_ref, up_ref, down_ref, out_ref):
    out_ref[0] = jnp.dot(a_ref[...], up_ref[...], preferred_element_type=jnp.float32)
    out_ref[1] = jnp.dot(b_ref[...], down_ref[...], preferred_element_type=jnp.float32)


def project_kernel(codes, moved, early, a_ref, b_ref, *rest):
    if early:
        early_ref, rest = rest[0], rest[1:]
    number = (1 if early else 2) * len(codes)
    w_refs, rest = rest[:number], rest[number:]
    if moved:
        held_ref, rest = rest[0], rest[1:]
    me = place()

    def put(at, c):
        for low, ref in zip((SEND, KEEP, HOLD), rest):

            @pl.when((at >= low) & (at < low + ref.shape[0]))
            def _():
                ref[at - low] = c

    for i, values in enumerate(moved):
        put(lookup(values, me), held_ref[i])
    for i, values in enumerate(codes):
        if early:
            x_ref = a_ref if i % 2 else b_ref
            c = early_ref[i]
            c += jnp.dot(x_ref[...], w_refs[i][...], preferred_element_type=jnp.float32)
        else:
            c = jnp.dot(a_ref[...], w_refs[2 * i][...], preferred_element_type=jnp.float32)
            c += jnp.dot(b_ref[...], w_refs[2 * i + 1][...], preferred_element_type=jnp.float32)
        put(lookup(values, me), c.astype(jnp.bfloat16))


def fold_kernel(codes, spans, per, *rest):
    kept, came, (own_ref, send_ref) = rest[: len(codes)], rest[len(codes) : -2], rest[-2:]
    me = place()
    for r, slots in enumerate(codes):
        cols = slice(*spans[r])
        for i, values in enumerate(slots):
            at = lookup(values, me)

            @pl.when(at != NONE)
            def _():
                c = kept[r][i].astype(jnp.float32) + came[r][i].astype(jnp.float32)
                c = c.astype(jnp.bfloat16)

                @pl.when(at < per)
                def _():
                    own_ref[at, :, cols] = c

                @pl.when(at >= per)
                def _():
                    send_ref[at - per, :, cols] = c


def finish_kernel(side, part_ref, *rest):
    out_ref, sem = rest[-2:]
    per, _, half = part_ref.shape
    core = (lax.axis_index("head") & 1) ^ side
    copies = []
    for part in range(per):
        start = pl.multiple_of((2 * part + core) * half, LANES)
        columns = out_ref.at[:, pl.ds(start, half)]
        copies.append(pltpu.make_async_copy(part_ref.at[part], columns, sem.at[part]))
        copies[-1].start()
    for copy in copies:
        copy.wait()


def reduce_plan(n, heads, sources, rounds):
    per = n // heads
    devices = [(s, h) for s in range(n) for h in range(heads)]
    caps = [max(1, n // 2 - len(rounds[1]))] + [len(places) for places in rounds[1:]]
    sources = [row + row[-1:] for row in sources]
    turns = {}
    for s in range(n):
        for owners in (0, 2):
            room = list(caps)
            for r, places in enumerate(rounds):
                for p in places:
                    if (sources[s][p] // per) & 2 == owners:
                        at = next(k for k in (r, *range(r + 1, 2)) if room[k])
                        room[at] -= 1
                        turns[s, p] = at
    plan = []
    held = {d: [] for d in devices}
    for r, places in enumerate(rounds):
        codes, moved = [[] for _ in places], [[] for _ in range(max(map(len, held.values())))]
        kept, later = {d: [] for d in devices}, {d: [] for d in devices}
        for s, h in devices:
            sent = 0
            jobs = [(moved[i], p) for i, p in enumerate(held[s, h])]
            jobs += [(codes[i], p) for i, p in enumerate(places)]
            for row, p in jobs:
                block = sources[s][p]
                away = (block // per) ^ h
                if turns[s, p] > r:
                    row.append(HOLD + len(later[s, h]))
                    later[s, h].append(p)
                elif away & 2:
                    row.append(SEND + sent)
                    sent += 1
                else:
                    row.append(KEEP + len(kept[s, h]))
                    kept[s, h].append(block % per + per * (away & 1))
            for row in moved[len(held[s, h]) :]:
                row.append(NONE)
        held = later
        ends = [[v[i] if i < len(v) else NONE for v in kept.values()] for i in range(caps[r])]
        plan.append((codes, moved, caps[r], max(map(len, held.values())), ends))
    return plan


def ring_device(n, heads, queries, keys, values, doc_ids, span_order, out_weight):
    tok_rows = queries.shape[0]
    span = tok_rows // 2
    group = queries.shape[1] // DH
    width = out_weight.shape[1]
    per = n // heads
    hops = n // 2
    ring = ring_order(n)
    where = {s: i for i, s in enumerate(ring)}
    sources = []
    for s in range(n):
        row = [s]
        for hop in range(1, hops):
            row += [ring[(where[s] - hop) % n], ring[(where[s] + hop) % n]]
        sources.append(row + [ring[(where[s] + hops) % n]])

    def gather(pieces):
        def move(way, x):
            step = 1 if way == "up" else -1
            pairs = [(ring[p], ring[(p + step) % n]) for p in range(n)]
            return lax.ppermute(x, "seq", pairs)

        ups, downs = list(pieces), list(pieces)
        got = [list(pieces)]
        for _ in range(1, hops):
            for i in range(len(pieces)):
                ups[i] = move("up", ups[i])
                downs[i] = move("dn", downs[i])
            got += [list(ups), list(downs)]
        if len(pieces) == 1:
            rows = pieces[0].shape[0] // 2
            parts = [(ups[0][:rows], downs[0][rows:])]
        else:
            cols = pieces[0].shape[1] // 2
            parts = [(ups[0][:, :cols], downs[1][:, :cols]), (ups[0][:, cols:], downs[1][:, cols:])]
        for up, down in parts:
            got.append([move("up", up), move("dn", down)])
        return got

    half = width // 2
    both = jnp.concatenate([keys, values], axis=1)
    left, right, both = lax.optimization_barrier(
        (out_weight[:, :half], out_weight[:, half:], both)
    )
    kv = gather([both])
    first = (lax.axis_index("head") & 1) == 0
    mine, other = jnp.where(first, left, right), jnp.where(first, right, left)
    beside = [(h, h ^ 1) for h in range(heads)]
    other = lax.ppermute(other, "head", beside)
    w = gather([mine, other])

    def attend(stage, slots, state, out_shape):
        first = stage == 0
        block = pltpu.VMEM((group * span, span), jnp.float32)
        states = pltpu.VMEM((2, group * span, span), jnp.float32)
        share = 2 * len(slots) * group * tok_rows * tok_rows
        args = [queries] + [piece for i in slots for piece in kv[i]] + state
        return pl.pallas_call(
            functools.partial(
                attention_kernel,
                n,
                span,
                group,
                [[row[i] for i in slots] for row in sources],
                first,
            ),
            out_shape=out_shape,
            in_specs=[SMEM, SMEM] + [VMEM] * (1 + len(args)),
            out_specs=jax.tree.map(lambda _: VMEM, out_shape),
            scratch_shapes=[
                pltpu.VMEM((len(slots), group * span, 2 * span), jnp.float32),
                block,
                pltpu.VMEM((2 * len(slots), span, 2 * DH), jnp.bfloat16),
                pltpu.SMEM((2 * len(slots) + 1,), jnp.int32),
                pltpu.SMEM((2 * len(slots) + 1,), jnp.int32),
            ]
            + ([] if first else [states, states]),
            compiler_params=limit(16),
            cost_estimate=pl.CostEstimate(
                flops=2 * share * DH,
                bytes_accessed=len(slots) * tok_rows * 4 * DH,
                transcendentals=share,
            ),
            name="attend",
        )(span_order, doc_ids, doc_ids.reshape(-1, span), *args)

    memory = jax.ShapeDtypeStruct((2, group * span, span), jnp.float32)
    state = attend(0, range(n - 1), [], (memory,) * 3)
    attended = attend(
        1, [n - 1], list(state), jax.ShapeDtypeStruct((tok_rows, group * DH), jnp.bfloat16)
    )
    paired = lax.ppermute(attended, "head", beside)

    def block(count, cols):
        return jax.ShapeDtypeStruct((count, tok_rows, cols), jnp.bfloat16)

    rounds = [list(range(n - 3)), [n - 3, n - 2], [n - 1], [n]]
    quarter = half // 2
    spans = [(0, half), (0, half), (0, quarter), (quarter, half)]
    across = [(h, h ^ 2) for h in range(heads)]
    kept, came, ends, held = [], [], [], []
    for r, (codes, moved, count, hold, end) in enumerate(
        reduce_plan(n, heads, sources, rounds)
    ):
        pieces = [piece for p in rounds[r] for piece in w[p]]
        begun = []
        if r == 1:
            (first_up, last_up), (last_down, first_down) = w[n - 3], w[n - 2]
            pieces = [last_up, last_down]
            begun = [
                pl.pallas_call(
                    early_kernel,
                    out_shape=jax.ShapeDtypeStruct((2, tok_rows, half), jnp.float32),
                    in_specs=[VMEM] * 4,
                    out_specs=VMEM,
                    compiler_params=limit(8),
                    name="early",
                )(attended, paired, first_up, first_down)
            ]
        cols = spans[r][1] - spans[r][0]
        outs = (block(count, cols),) * 2 + ((block(hold, cols),) if hold else ())
        send, keep, *rest = pl.pallas_call(
            functools.partial(project_kernel, codes, moved, r == 1),
            out_shape=outs,
            in_specs=[VMEM] * (2 + len(begun) + len(pieces) + len(held)),
            out_specs=(VMEM,) * len(outs),
            compiler_params=limit(8),
            cost_estimate=pl.CostEstimate(
                flops=2 * tok_rows * group * DH * cols * len(pieces),
                bytes_accessed=2 * group * DH * cols * len(pieces),
                transcendentals=0,
            ),
            name="project",
        )(attended, paired, *begun, *pieces, *held)
        came.append(lax.ppermute(send, "head", across))
        held = rest
        kept.append(keep)
        ends.append(end)

    own, send = pl.pallas_call(
        functools.partial(fold_kernel, ends, spans, per),
        out_shape=(block(per, half),) * 2,
        in_specs=[VMEM] * (2 * len(ends)),
        out_specs=(VMEM, VMEM),
        compiler_params=limit(8),
        name="fold",
    )(*kept, *came)
    joined = lax.ppermute(send, "head", beside)

    def finish(side, part, *out):
        return pl.pallas_call(
            functools.partial(finish_kernel, side),
            out_shape=jax.ShapeDtypeStruct((tok_rows, per * width), jnp.bfloat16),
            in_specs=[VMEM] + [HBM] * len(out),
            out_specs=HBM,
            input_output_aliases={1: 0} if out else {},
            scratch_shapes=[pltpu.SemaphoreType.DMA((per,))],
            compiler_params=limit(4),
            name="finish",
        )(part, *out)

    return finish(1, joined, finish(0, own))


def on_device(queries, keys, values, doc_ids, span_order, out_weight):
    tok_rows = queries.shape[0]
    span = tok_rows // 2
    local_heads = queries.shape[1] // DH
    local_kv = keys.shape[1] // DH
    group_size = local_heads // local_kv
    n_blocks = span_order.shape[0]
    scale = 1.0 / math.sqrt(DH)
    mine = lax.axis_index("seq")
    own_blocks = lax.dynamic_slice_in_dim(span_order, 2 * mine, 2, 0)
    local_rows = jnp.arange(tok_rows, dtype=jnp.int32)
    qpos = jnp.where(local_rows < span, own_blocks[0], own_blocks[1]) * span + local_rows % span
    qdoc = jnp.take(doc_ids, qpos)
    q_heads = queries.reshape(tok_rows, local_kv, group_size, DH)

    def update(state, kblk, vblk, kpos, kdoc):
        largest, total, summed = state
        count = kblk.shape[0]
        k_heads = kblk.reshape(count, local_kv, DH)
        v_heads = vblk.reshape(count, local_kv, DH)
        scores = (
            jnp.einsum("qhgd,khd->hgqk", q_heads, k_heads, preferred_element_type=jnp.float32)
            * scale
        )
        visible = (qdoc[:, None] == kdoc[None, :]) & (kpos[None, :] <= qpos[:, None])
        masked = jnp.where(visible, scores, jnp.float32(-1e30))
        new_largest = jnp.maximum(largest, jnp.max(masked, axis=-1))
        factor = jnp.exp(largest - new_largest)
        weights = jnp.where(visible, jnp.exp(masked - new_largest[..., None]), jnp.float32(0.0))
        total = total * factor + jnp.sum(weights, axis=-1)
        weights_b = weights.astype(jnp.bfloat16)
        added = jnp.einsum("hgqk,khd->qhgd", weights_b, v_heads, preferred_element_type=jnp.float32)
        summed = summed * jnp.transpose(factor, (2, 0, 1))[..., None] + added
        return (new_largest, total, summed)

    initial = (
        jnp.full((local_kv, group_size, tok_rows), -1e30, jnp.float32),
        jnp.zeros((local_kv, group_size, tok_rows), jnp.float32),
        jnp.zeros((tok_rows, local_kv, group_size, DH), jnp.float32),
    )
    state = initial
    kpiece = lax.all_gather(keys, "seq", axis=0, tiled=True)
    vpiece = lax.all_gather(values, "seq", axis=0, tiled=True)
    count = kpiece.shape[0]
    width = math.gcd(count, 1024)
    steps = count // width
    rows = jnp.arange(count, dtype=jnp.int32)
    match = (rows // span)[:, None] == jnp.arange(n_blocks, dtype=jnp.int32)[None, :]
    owner = jnp.sum(jnp.where(match, span_order[None, :], 0), axis=1)
    kpos = owner * span + rows % span
    kdoc = jnp.take(doc_ids, kpos)
    kparts = kpiece.reshape(steps, width, kpiece.shape[1])
    vparts = vpiece.reshape(steps, width, vpiece.shape[1])

    def one_step(carry, items):
        kblk, vblk, pblk, dblk = items
        carry = update(carry, kblk, vblk, pblk, dblk)
        return (carry, None)

    state, _ = lax.scan(
        one_step, state, (kparts, vparts, kpos.reshape(steps, width), kdoc.reshape(steps, width))
    )
    _, total, summed = state
    attended = (summed / jnp.transpose(total, (2, 0, 1))[..., None]).astype(jnp.bfloat16)
    attended = attended.reshape(tok_rows, local_heads * DH)
    partial_out = jnp.dot(
        attended,
        lax.all_gather(out_weight, "seq", axis=1, tiled=True),
        preferred_element_type=jnp.float32,
    )
    return lax.psum_scatter(
        partial_out.astype(jnp.bfloat16), "head", scatter_dimension=1, tiled=True
    )


def solution(mesh):
    n, heads = mesh.shape["seq"], mesh.shape["head"]

    def on_each(queries, keys, values, doc_ids, span_order, out_weight):
        span = queries.shape[0] // 2
        ring = (
            4 <= n <= 16
            and n % 2 == 0
            and n % heads == 0
            and heads == 4
            and keys.shape[1] == DH
            and span % LANES == 0
            and out_weight.shape[1] % (4 * LANES) == 0
        )
        args = (queries, keys, values, doc_ids, span_order, out_weight)
        if not ring:
            return on_device(*args)
        return ring_device(n, heads, *args)

    return jax.shard_map(
        on_each,
        mesh=mesh,
        in_specs=(P("seq", "head"), P("seq", "head"), P("seq", "head"), P(), P(), P("head", "seq")),
        out_specs=P("seq", "head"),
        check_vma=False,
    )
```
